256 devices in a mesh: groups: 2 (over y), gx: 32 (over z, core), gy: 4 (over x).
Axes of the slice: x: 4, y: 2, z: 16, core: 2. Of those that a mesh axis runs over, the one named last changes fastest.
The devices are a block of a 4x16x16 slice.
Arguments:
- hidden_in: bfloat16 [1024, 18432], P(('groups', 'gx'), 'gy'), parts along dimension 0, may hold values from -6 to 6
- w_query: bfloat16 [18432, 12288], P('gy', 'gx'), may hold values from -0.046875 to 0.046875
- w_out: bfloat16 [12288, 18432], P('gx', 'gy'), may hold values from -0.4375 to 0.4375
- cache_keys: bfloat16 [1024, 1024, 256], P(('groups', 'gx', 'gy')), parts along dimension 0, may hold values from -250 to 250
- cache_values: bfloat16 [1024, 1024, 256], P(('groups', 'gx', 'gy')), parts along dimension 0, may hold values from -6 to 6
- lengths: int32 [1024], P(('groups', 'gx', 'gy')), parts along dimension 0, may hold values from 128 to 1024
Outputs:
- layer_out: bfloat16 [1024, 18432], P(('groups', 'gx'), 'gy'), parts along dimension 0
The draws below stay inside these ranges and needn't reach their ends.
There are 2 independent parts, one for each index of `groups`. The reference program is written for one: setup_inputs(seed, part) draws one part's arguments, and reference() takes and returns one part's arrays. A program takes and returns all parts, laid end to end along the dimension named above; an argument that names none is the same for every part. Nothing has to cross between parts.
All inputs are finite; a program needn't handle non-finite values.
Results may differ from the reference program's by a relative error of at most 0.0097.
Values may be sent and summed in bfloat16 or wider, within the bound.
A program may use at most 64 MiB of HBM per device.

```python
import jax
import jax.numpy as jnp
from jax import lax

D = 18432
HEADS = 48
HD = 256
QW = 12288
SEQ_DEV = 4
LMAX = 1024
B = 512


def draw_cache_keys(key, part):
    base = jnp.clip(jax.random.normal(jax.random.fold_in(key, 11), (B, LMAX, HD), jnp.float32), -6.0, 6.0)
    return base.astype(jnp.bfloat16)


def touch_ends(drawn, own_key, smallest, high):
    longest = drawn.shape.index(max(drawn.shape))
    spots = []
    for shift in (0, 1):
        where = [jax.random.randint(jax.random.fold_in(own_key, axis), (), 0, length) for axis, length in enumerate(drawn.shape)]
        where[longest] = (where[longest] + shift) % drawn.shape[longest]
        spots.append(tuple(where))
    return drawn.at[spots[0]].set(smallest).at[spots[1]].set(high)


def levels(own_key, dims, pieces, least, high):
    loudness, own = 1.0, jax.random.fold_in(own_key, 6)
    for dim, shards_of in pieces:
        draws = jnp.exp(jax.random.uniform(jax.random.fold_in(own, dim), (shards_of,), jnp.float32, least / len(pieces), high / len(pieces)))
        loudness = loudness * jnp.repeat(draws, dims[dim] // shards_of).reshape([-1 if axis == dim else 1 for axis in range(len(dims))])
    return loudness


def normal_values(own_key, dims, spread, most, cuts=(), held_as=jnp.bfloat16):
    drawn = jax.random.normal(own_key, dims, jnp.float32) * spread
    if len(cuts) > 0:
        drawn = levels(own_key, dims, cuts, -0.22, 0.18) * drawn
    return jnp.clip(drawn, min=-most, max=most).astype(held_as)


def setup_inputs(seed: int = 0, part: int = 0) -> dict:
    splits = jax.random.split(jax.random.key(seed), 7)
    own_keys = jax.random.split(jax.random.fold_in(splits[6], part), 7)
    return {
        "hidden_in": normal_values(own_keys[0], (B, D), 1.0, 6.0, ((0, 32), (1, 4))),
        "w_query": normal_values(splits[1], (D, QW), D ** -0.5, 0.046875, ((0, 4), (1, 32))),
        "w_out": normal_values(splits[2], (QW, D), (QW // 64) ** -0.5, 0.4375, ((0, 32), (1, 4))),
        "cache_keys": draw_cache_keys(jax.random.fold_in(jax.random.fold_in(splits[6], part), 71), part),
        "cache_values": normal_values(own_keys[4], (B, LMAX, HD), 1.0, 6.0, ((0, 128),)),
        "lengths": touch_ends(jax.random.randint(own_keys[5], (B,), LMAX // 8, LMAX + 1), jax.random.fold_in(own_keys[5], 1), LMAX // 8, LMAX).astype(jnp.int32),
    }


def attend(operands):
    query_block, key_block, value_block, length_block = operands
    scores = jnp.einsum('bhd,bld->bhl', query_block.astype(jnp.float32), key_block.astype(jnp.float32)) / jnp.sqrt(jnp.float32(HD))
    live_slots = jnp.arange(LMAX)[None, None, :] < length_block[:, None, None]
    scores = jnp.where(live_slots, scores, jnp.float32(-1e+30))
    top_score = lax.optimization_barrier(jnp.max(scores, axis=2, keepdims=True))
    expo = jnp.where(live_slots, jnp.exp(scores - top_score), jnp.float32(0.0))
    probs = (expo / lax.optimization_barrier(jnp.sum(expo, axis=2, keepdims=True))).astype(jnp.bfloat16)
    mixed = jnp.einsum('bhl,bld->bhd', probs.astype(jnp.float32), value_block.astype(jnp.float32))
    return mixed.astype(jnp.bfloat16)

def reference(hidden_in, w_query, w_out, cache_keys, cache_values, lengths):
    query = jnp.dot(hidden_in, w_query, preferred_element_type=jnp.float32).astype(jnp.bfloat16)
    blocks = B // SEQ_DEV
    query_heads = query.reshape(blocks, SEQ_DEV, HEADS, HD)
    key_blocks = cache_keys.reshape(blocks, SEQ_DEV, LMAX, HD)
    value_blocks = cache_values.reshape(blocks, SEQ_DEV, LMAX, HD)
    length_blocks = lengths.reshape(blocks, SEQ_DEV)
    attended = lax.map(attend, (query_heads, key_blocks, value_blocks, length_blocks))
    attended = attended.reshape(B, QW)
    return jnp.dot(attended, w_out, preferred_element_type=jnp.float32).astype(jnp.bfloat16)
```

```python
import functools

import jax
import jax.numpy as jnp
from jax import lax
from jax.experimental import pallas as pl
from jax.experimental.pallas import tpu as pltpu
from jax.sharding import PartitionSpec as P

MESH = pl.DeviceIdType.MESH
CORES = 2
IN_CHUNKS = 4
OUT_CHUNKS = 6
F32 = jnp.float32
BF16 = jnp.bfloat16


def source_offset(u, half):
    return half - (u + 1) // 2 if u % 2 else half + u // 2


def kernel(
    nz,
    nx,
    lengths,
    hidden,
    w_query,
    w_out,
    keys,
    values,
    out,
    gathered,
    wq,
    wo,
    k_buf,
    v_buf,
    acc,
    part,
    part_in,
    q_send,
    q_in,
    q_wide,
    att_wide,
    att_send,
    att_in,
    att,
    sums,
    sums_in,
    last,
    local_sem,
    ring_send_sem,
    ring_sem,
    pair_send_sem,
    pair_sem,
    part_send_sem,
    part_sem,
    q_send_sem,
    q_sem,
    att_send_sem,
    att_sem,
    rows_send_sem,
    rows_sem,
    swap_send_sem,
    swap_sem,
    wo_send_sem,
    wo_sem,
    sums_send_sem,
    sums_sem,
    last_send_sem,
    last_sem,
):
    half = nz // 2
    gx = lax.axis_index("gx")
    x = lax.axis_index("gy")
    z = gx // CORES
    c = gx % CORES
    other = 1 - c
    seqs, slots, hd = k_buf.shape
    width = hidden.shape[1]
    cols = width // IN_CHUNKS
    own_cols = width // CORES
    out_cols = own_cols // OUT_CHUNKS
    feats = w_query.shape[1]
    block = nx * seqs

    def at_z(chip, core):
        return {"gx": lax.rem(chip + 2 * nz, nz) * CORES + core}

    def at_x(offset):
        return {"gy": lax.rem(x + offset, nx)}

    side = (at_z(z + 1, c), at_z(z - 1, c))
    pair = {"gx": z * CORES + other}

    def remote(src, dst, send_sem, recv_sem, device):
        return pltpu.make_async_remote_copy(
            src_ref=src, dst_ref=dst, send_sem=send_sem, recv_sem=recv_sem, device_id=device, device_id_type=MESH
        )

    def half_cols(core):
        return pl.ds(pl.multiple_of(core * own_cols, 128), own_cols)

    own_slot = gathered.at[half - 1, CORES + c]
    loads = [
        pltpu.make_async_copy(hidden, own_slot, local_sem.at[0]),
        pltpu.make_async_copy(w_query, wq, local_sem.at[1]),
        pltpu.make_async_copy(w_out.at[:, half_cols(c)], wo.at[c], local_sem.at[2]),
        pltpu.make_async_copy(keys, k_buf, local_sem.at[3]),
        pltpu.make_async_copy(values, v_buf, local_sem.at[4]),
    ]
    loads[0].start()
    loads[1].start()

    barrier = pltpu.get_barrier_semaphore()
    greeted = [*side, pair] + [at_x(k) for k in range(1, nx)]
    for device in greeted:
        pl.semaphore_signal(barrier, inc=1, device_id=device, device_id_type=MESH)
    pl.semaphore_wait(barrier, len(greeted))
    loads[0].wait()

    def piece(j):
        return pl.ds(j * cols, cols)

    def home(s, d):
        return 0 if isinstance(s, int) and s == half - 1 else d

    def ring(d, s, j):
        src = own_slot if isinstance(s, int) and s == 0 else gathered.at[s - 1, CORES * d + c]
        dst = gathered.at[s, CORES * home(s, d) + c]
        return remote(src.at[:, piece(j)], dst.at[:, piece(j)], ring_send_sem.at[d, s], ring_sem.at[d, s, j], side[d])

    def to_pair(d, s, j):
        ref = gathered.at[s, CORES * home(s, d) + c, :, piece(j)]
        return remote(ref, ref, pair_send_sem.at[home(s, d), s], pair_sem.at[home(s, d), s], pair)

    def travels(d, s, j):
        return s < half - 1 or (j < IN_CHUNKS // 2) == (d == 0)

    def dot_piece(s, j):
        if j == 0:
            for d in range(2):
                ref = gathered.at[s, CORES * d + other]
                remote(ref, ref, pair_send_sem.at[d, s], pair_sem.at[d, s], pair).wait_recv()
        lhs = gathered[s, :, :, j * cols : (j + 1) * cols].reshape(2 * CORES * block, cols)
        term = jnp.dot(lhs, wq[j * cols : (j + 1) * cols, :], preferred_element_type=F32)
        if j == 0:
            acc[...] = term
        else:
            acc[...] += term

    def send_parts(s):
        for g in range(nx):
            part[s, g] = jnp.concatenate(
                [acc[b * block + g * seqs : b * block + (g + 1) * seqs, :] for b in range(2 * CORES)], axis=0
            )
        for k in range(1, nx):
            part_copy(s, k).start()

    def part_copy(s, k):
        return remote(
            part.at[s, lax.rem(x + k, nx)], part_in.at[s, k - 1], part_send_sem.at[s, k - 1], part_sem.at[s, k - 1], at_x(k)
        )

    def q_copy(s, d, r):
        core = lax.rem(c + r, CORES)
        if isinstance(s, int) and s == half - 1:
            chip = z + half if d == 0 else z
        else:
            chip = z - 1 - s if d == 0 else z + 1 + s
        return remote(q_send.at[s, CORES * d + core], q_in.at[gx], q_send_sem, q_sem.at[gx], at_z(chip, core))

    def send_queries(s):
        total = part[s, x]
        for k in range(1, nx):
            part_copy(s, k).wait_recv()
            total = total + part_in[s, k - 1]
        for b in range(2 * CORES):
            q_send[s, b] = total[b * seqs : (b + 1) * seqs, :].astype(BF16)
        for d in range(2):
            for r in range(CORES):
                if isinstance(s, int) and s == half - 1 and d == 1 and r == 0:
                    q_in[gx] = q_send[s, CORES + c]
                else:
                    q_copy(s, d, r).start()

    for j in range(IN_CHUNKS):
        for d in range(2):
            if travels(d, 0, j):
                ring(d, 0, j).start()
    for j in range(IN_CHUNKS):
        ref = own_slot.at[:, piece(j)]
        remote(ref, ref, pair_send_sem.at[1, half - 1], pair_sem.at[1, half - 1], pair).start()
    loads[1].wait()
    for load in loads[2:]:
        load.start()
    wo_copy = remote(w_out.at[:, half_cols(other)], wo.at[c], wo_send_sem, wo_sem, pair)
    wo_copy.start()

    def gather_step(s):
        known = isinstance(s, int)
        for j in range(IN_CHUNKS):
            for d in range(2):
                if not known or travels(d, s, j):
                    ring(d, s, j).wait_recv()
                    if not known or (s < half - 1 and travels(d, s + 1, j)):
                        ring(d, s + 1, j).start()
                    to_pair(d, s, j).start()
            if known:
                if s >= 1:
                    dot_piece(s - 1, j)
            else:
                pl.when(s >= 1)(functools.partial(dot_piece, s - 1, j))
        if known:
            if s >= 1:
                send_parts(s - 1)
            if s >= 2:
                send_queries(s - 2)
        else:
            pl.when(s >= 1)(functools.partial(send_parts, s - 1))
            pl.when(s >= 2)(functools.partial(send_queries, s - 2))

    gather_step(0)

    @pl.loop(1, half - 2)
    def _(s):
        gather_step(s)

    for s in range(max(half - 2, 1), half):
        gather_step(s)
    for j in range(IN_CHUNKS):
        dot_piece(half - 1, j)
    send_parts(half - 1)
    send_queries(half - 2)
    send_queries(half - 1)

    for load in loads[3:]:
        load.wait()

    @pl.loop(1, nz * CORES)
    def _(k):
        ref = q_in.at[lax.rem(gx + k, nz * CORES)]
        remote(ref, ref, q_send_sem, q_sem.at[lax.rem(gx + k, nz * CORES)], pair).wait_recv()

    q_wide[...] = q_in[...].reshape(nz, CORES, seqs, feats).astype(F32)
    heads = CORES * feats // hd
    for i in range(seqs):
        rows = jnp.concatenate([q_wide[:, core, i, :] for core in range(CORES)], axis=1)
        query = jnp.concatenate([rows[:, h * hd : (h + 1) * hd] for h in range(heads)], axis=0).astype(BF16)
        scores = lax.dot_general(query, k_buf[i], (((1,), (1,)), ((), ())), preferred_element_type=F32)
        scores = scores * F32(hd**-0.5)
        live = lax.broadcasted_iota(jnp.int32, scores.shape, 1) < lengths[i]
        scores = jnp.where(live, scores, F32(-1e30))
        expo = jnp.where(live, jnp.exp(scores - jnp.max(scores, axis=1, keepdims=True)), F32(0.0))
        probs = (expo / jnp.sum(expo, axis=1, keepdims=True)).astype(BF16)
        mixed = jnp.dot(probs, v_buf[i], preferred_element_type=F32)
        wide = jnp.concatenate([mixed[h * nz : (h + 1) * nz, :] for h in range(heads)], axis=1)
        for core in range(CORES):
            att_wide[:, core, i, :] = wide[:, core * feats : (core + 1) * feats]
    att_send[...] = att_wide[...].astype(BF16)

    def att_copy(u, r):
        core = lax.rem(c + r, CORES)
        chip = lax.rem(z - source_offset(u, half) + nz, nz)
        return remote(att_send.at[chip, core], att_in.at[x, u, c], att_send_sem, att_sem.at[u, c], at_z(chip, core))

    for u in range(nz):
        for r in range(CORES):
            if u == nz - 1 and r == 0:
                att_in[x, u, c] = att_send[z, c]
            else:
                att_copy(u, r).start()

    per = nz // 4
    batches = [(b * per, (b + 1) * per) for b in range(4)]

    def rows_copy(b, k):
        ref = att_in.at[x, batches[b][0] : batches[b][1]]
        return remote(ref, ref, rows_send_sem.at[b, k - 1], rows_sem.at[b, k - 1], at_x(k))

    def swap_copy(b):
        ref = att.at[c, batches[b][0] : batches[b][1]]
        return remote(ref, ref, swap_send_sem.at[b], swap_sem.at[b], pair)

    for b in range(4):
        for u in range(*batches[b]):
            for r in range(CORES):
                core = lax.rem(c + r, CORES)
                if u < nz - 1 or r > 0:
                    ref = att_in.at[x, u, core]
                    remote(ref, ref, att_send_sem, att_sem.at[u, core], pair).wait_recv()
        for k in range(1, nx):
            rows_copy(b, k).start()
    for b in range(4):
        for k in range(1, nx):
            rows_copy(b, k).wait_recv()
        for u in range(*batches[b]):
            for core in range(CORES):
                att[c, u, core] = jnp.concatenate(
                    [att_in[g, u, core].astype(F32) for g in range(nx)], axis=0
                ).astype(BF16)
        swap_copy(b).start()
    loads[2].wait()
    wo_copy.wait_recv()
    for b in range(4):
        swap_copy(b).wait_recv()

    def out_piece(j):
        return pl.ds(j * out_cols, out_cols)

    def projected(u, count, j):
        lhs = jnp.concatenate(
            [att[f, pl.ds(u, count)].reshape(count * CORES * block, feats) for f in range(CORES)], axis=1
        )
        rhs = wo[:, :, j * out_cols : (j + 1) * out_cols].reshape(CORES * feats, out_cols)
        return jnp.dot(lhs, rhs, preferred_element_type=F32)

    def sums_copy(d, s, j):
        return remote(
            sums.at[d, s, :, out_piece(j)],
            sums_in.at[d, s, :, out_piece(j)],
            sums_send_sem.at[d, s],
            sums_sem.at[d, s, j],
            side[d],
        )

    def starts(d, j):
        return (j < OUT_CHUNKS // 2) == (d == 0)

    tall = CORES * block

    def out_step(s):
        known = isinstance(s, int)
        for j in range(OUT_CHUNKS):
            span = slice(j * out_cols, (j + 1) * out_cols)
            if known and s == 0:
                d = 0 if starts(0, j) else 1
                sums[d, 0, :, span] = projected(0, 1, j).astype(BF16)
                sums_copy(d, 0, j).start()
                continue
            both = projected(2 * s - 1, 2, j)
            for d in range(2):
                term = both[d * tall : (d + 1) * tall]
                if not known or s > 1 or starts(d, j):
                    sums_copy(d, s - 1, j).wait_recv()
                    term = term + sums_in[d, s - 1, :, span].astype(F32)
                sums[d, s, :, span] = term.astype(BF16)
                sums_copy(d, s, j).start()

    out_step(0)
    out_step(1)

    @pl.loop(2, half)
    def _(s):
        out_step(s)

    def last_copy(j):
        own = pl.ds(pl.multiple_of(c * own_cols + j * out_cols, 128), out_cols)
        return remote(
            last.at[other, :, out_piece(j)], out.at[:, own], last_send_sem.at[j], last_sem.at[j], pair
        )

    for j in range(OUT_CHUNKS):
        span = slice(j * out_cols, (j + 1) * out_cols)
        term = projected(nz - 1, 1, j)
        for d in range(2):
            sums_copy(d, half - 1, j).wait_recv()
            term = term + sums_in[d, half - 1, :, span].astype(F32)
        for core in range(CORES):
            last[core, :, span] = term[core * block : (core + 1) * block].astype(BF16)
        last_copy(j).start()
    out[:, half_cols(c)] = last[c]
    for j in range(OUT_CHUNKS):
        last_copy(j).wait_recv()

    def ring_sent(d, s, whole):
        ref = gathered.at[0, c] if whole else gathered.at[0, c, :, pl.ds(0, width // 2)]
        remote(ref, ref, ring_send_sem.at[d, s], ring_sem.at[d, s, 0], side[d]).wait_send()

    def pair_sent(d, s):
        ref = gathered.at[0, c]
        remote(ref, ref, pair_send_sem.at[d, s], pair_sem.at[d, s], pair).wait_send()

    @pl.loop(0, half)
    def _(s):
        for d in range(2):
            pair_sent(d, s)
        for k in range(1, nx):
            part_copy(s, k).wait_send()

    @pl.loop(0, half - 1)
    def _(s):
        for d in range(2):
            ring_sent(d, s, True)

    @pl.loop(1, half)
    def _(s):
        for d in range(2):
            ref = sums.at[d, s]
            remote(ref, ref, sums_send_sem.at[d, s], sums_sem.at[d, s, 0], side[d]).wait_send()

    for d in range(2):
        ring_sent(d, half - 1, False)
        ref = sums.at[d, 0, :, pl.ds(0, own_cols // 2)]
        remote(ref, ref, sums_send_sem.at[d, 0], sums_sem.at[d, 0, 0], side[d]).wait_send()
    ref = q_in.at[pl.ds(0, nz * CORES - 1)]
    remote(ref, ref, q_send_sem, q_sem.at[0], pair).wait_send()
    remote(ref, ref, att_send_sem, att_sem.at[0, 0], pair).wait_send()
    for b in range(4):
        swap_copy(b).wait_send()
        for k in range(1, nx):
            rows_copy(b, k).wait_send()
    wo_copy.wait_send()
    for j in range(OUT_CHUNKS):
        last_copy(j).wait_send()


def solution(mesh):
    nz = mesh.shape["gx"] // CORES
    nx = mesh.shape["gy"]
    half = nz // 2

    def body(hidden_in, w_query, w_out, cache_keys, cache_values, lengths):
        block, width = hidden_in.shape
        feats = w_query.shape[1]
        seqs, slots, hd = cache_keys.shape
        own_cols = width // CORES
        dma = pltpu.SemaphoreType.DMA
        hbm = pl.BlockSpec(memory_space=pltpu.HBM)
        return pl.pallas_call(
            functools.partial(kernel, nz, nx),
            out_shape=jax.ShapeDtypeStruct((block, width), BF16),
            in_specs=[pl.BlockSpec(memory_space=pltpu.SMEM)] + [hbm] * 5,
            out_specs=pl.BlockSpec(memory_space=pltpu.VMEM),
            scratch_shapes=[
                pltpu.VMEM((half, 2 * CORES, block, width), BF16),
                pltpu.VMEM(w_query.shape, BF16),
                pltpu.VMEM((CORES, feats, own_cols), BF16),
                pltpu.VMEM(cache_keys.shape, BF16),
                pltpu.VMEM(cache_values.shape, BF16),
                pltpu.VMEM((2 * CORES * block, feats), F32),
                pltpu.VMEM((half, nx, 2 * CORES * seqs, feats), F32),
                pltpu.VMEM((half, nx - 1, 2 * CORES * seqs, feats), F32),
                pltpu.VMEM((half, 2 * CORES, seqs, feats), BF16),
                pltpu.VMEM((nz * CORES, seqs, feats), BF16),
                pltpu.VMEM((nz, CORES, seqs, feats), F32),
                pltpu.VMEM((nz, CORES, seqs, feats), F32),
                pltpu.VMEM((nz, CORES, seqs, feats), BF16),
                pltpu.VMEM((nx, nz, CORES, seqs, feats), BF16),
                pltpu.VMEM((CORES, nz, CORES, block, feats), BF16),
                pltpu.VMEM((2, half, CORES * block, own_cols), BF16),
                pltpu.VMEM((2, half, CORES * block, own_cols), BF16),
                pltpu.VMEM((CORES, block, own_cols), BF16),
                dma((5,)),
                dma((2, half)),
                dma((2, half, IN_CHUNKS)),
                dma((2, half)),
                dma((2, half)),
                dma((half, nx - 1)),
                dma((half, nx - 1)),
                dma(()),
                dma((nz * CORES,)),
                dma(()),
                dma((nz, CORES)),
                dma((4, nx - 1)),
                dma((4, nx - 1)),
                dma((4,)),
                dma((4,)),
                dma(()),
                dma(()),
                dma((2, half)),
                dma((2, half, OUT_CHUNKS)),
                dma((OUT_CHUNKS,)),
                dma((OUT_CHUNKS,)),
            ],
            compiler_params=pltpu.CompilerParams(
                collective_id=0, has_side_effects=True, vmem_limit_bytes=60 * 2**20
            ),
            name="decode_step",
        )(lengths, hidden_in, w_query, w_out, cache_keys, cache_values)

    return jax.shard_map(
        body,
        mesh=mesh,
        in_specs=(
            P(("groups", "gx"), "gy"),
            P("gy", "gx"),
            P("gx", "gy"),
            P(("groups", "gx", "gy"), None, None),
            P(("groups", "gx", "gy"), None, None),
            P(("groups", "gx", "gy")),
        ),
        out_specs=P(("groups", "gx"), "gy"),
        check_vma=False,
    )
```

```python
import functools

import jax
import jax.numpy as jnp
from jax import lax
from jax.experimental import pallas as pl
from jax.experimental.pallas import tpu as pltpu
from jax.sharding import PartitionSpec as P

MESH = pl.DeviceIdType.MESH
CORES = 2
IN_CHUNKS = 6
OUT_CHUNKS = 9
PER_BATCH = 4
F32 = jnp.float32
BF16 = jnp.bfloat16


def source_offset(v, half):
    return 0 if v == 0 else half + v // 2 if v % 2 else half - v // 2


def kernel(
    nz,
    nx,
    lengths,
    hidden,
    w_query,
    w_out,
    keys,
    values,
    out,
    gathered,
    wq,
    wo,
    k_buf,
    v_buf,
    acc,
    part,
    part_in,
    q_send,
    q_in,
    q_wide,
    att_wide,
    att_send,
    att_in,
    att,
    sums,
    sums_in,
    last,
    local_sem,
    ring_send_sem,
    ring_sem,
    pair_send_sem,
    pair_sem,
    part_send_sem,
    part_sem,
    q_send_sem,
    q_sem,
    att_send_sem,
    att_sem,
    rows_send_sem,
    rows_sem,
    swap_send_sem,
    swap_sem,
    wo_send_sem,
    wo_sem,
    sums_send_sem,
    sums_sem,
    last_send_sem,
    last_sem,
):
    half = nz // 2
    gx = lax.axis_index("gx")
    x = lax.axis_index("gy")
    z = gx // CORES
    c = gx % CORES
    other = 1 - c
    seqs, slots, hd = k_buf.shape
    width = hidden.shape[1]
    cols = width // IN_CHUNKS
    own_cols = width // CORES
    out_cols = own_cols // OUT_CHUNKS
    feats = w_query.shape[1]
    block = nx * seqs

    def at_z(chip, core):
        return {"gx": lax.rem(chip + 2 * nz, nz) * CORES + core}

    def at_x(offset):
        return {"gy": lax.rem(x + offset, nx)}

    side = (at_z(z + 1, c), at_z(z - 1, c))
    pair = {"gx": z * CORES + other}

    def remote(src, dst, send_sem, recv_sem, device):
        return pltpu.make_async_remote_copy(
            src_ref=src, dst_ref=dst, send_sem=send_sem, recv_sem=recv_sem, device_id=device, device_id_type=MESH
        )

    def half_cols(core):
        return pl.ds(pl.multiple_of(core * own_cols, 128), own_cols)

    own_slot = gathered.at[half, c]
    loads = [
        pltpu.make_async_copy(hidden, own_slot, local_sem.at[0]),
        pltpu.make_async_copy(w_query, wq, local_sem.at[1]),
        pltpu.make_async_copy(w_out.at[:, half_cols(c)], wo.at[c], local_sem.at[2]),
        pltpu.make_async_copy(keys, k_buf, local_sem.at[3]),
        pltpu.make_async_copy(values, v_buf, local_sem.at[4]),
    ]
    loads[0].start()
    loads[1].start()

    barrier = pltpu.get_barrier_semaphore()
    greeted = [*side, pair] + [at_x(k) for k in range(1, nx)]
    for device in greeted:
        pl.semaphore_signal(barrier, inc=1, device_id=device, device_id_type=MESH)
    pl.semaphore_wait(barrier, len(greeted))
    loads[0].wait()

    def piece(j):
        return pl.ds(j * cols, cols)

    def home(s, d):
        return 0 if isinstance(s, int) and s == half - 1 else d

    def ring(d, s, j):
        src = own_slot if isinstance(s, int) and s == 0 else gathered.at[s - 1, CORES * d + c]
        dst = gathered.at[s, CORES * home(s, d) + c]
        return remote(src.at[:, piece(j)], dst.at[:, piece(j)], ring_send_sem.at[d, s], ring_sem.at[d, s, j], side[d])

    def to_pair(d, s, j):
        ref = gathered.at[s, CORES * home(s, d) + c, :, piece(j)]
        return remote(ref, ref, pair_send_sem.at[home(s, d), s], pair_sem.at[home(s, d), s], pair)

    def travels(d, s, j):
        return s < half - 1 or (j < IN_CHUNKS // 2) == (d == 0)

    def blocks(t):
        return CORES if isinstance(t, int) and t >= half - 1 else 2 * CORES

    def dot_piece(t, j):
        if j == 0:
            for d in range(blocks(t) // CORES):
                ref = gathered.at[t, CORES * d + other]
                remote(ref, ref, pair_send_sem.at[d, t], pair_sem.at[d, t], pair).wait_recv()
        tall = blocks(t) * block
        lhs = gathered[t, : blocks(t), :, j * cols : (j + 1) * cols].reshape(tall, cols)
        term = jnp.dot(lhs, wq[j * cols : (j + 1) * cols, :], preferred_element_type=F32)
        if j == 0:
            acc[:tall] = term
        else:
            acc[:tall] += term

    def part_copy(t, k):
        rows = pl.ds(0, blocks(t) * seqs)
        return remote(
            part.at[t, lax.rem(x + k, nx), rows],
            part_in.at[t, k - 1, rows],
            part_send_sem.at[t, k - 1],
            part_sem.at[t, k - 1],
            at_x(k),
        )

    def send_parts(t):
        for g in range(nx):
            part[t, g, : blocks(t) * seqs] = jnp.concatenate(
                [acc[b * block + g * seqs : b * block + (g + 1) * seqs, :] for b in range(blocks(t))], axis=0
            )
        for k in range(1, nx):
            part_copy(t, k).start()

    def q_copy(t, d, r):
        core = lax.rem(c + r, CORES)
        if isinstance(t, int) and t >= half - 1:
            chip = z if t == half else z + half
        else:
            chip = z - 1 - t if d == 0 else z + 1 + t
        return remote(q_send.at[t, CORES * d + core], q_in.at[gx], q_send_sem, q_sem.at[gx], at_z(chip, core))

    def send_queries(t):
        rows = blocks(t) * seqs
        total = part[t, x, :rows]
        for k in range(1, nx):
            part_copy(t, k).wait_recv()
            total = total + part_in[t, k - 1, :rows]
        for b in range(blocks(t)):
            q_send[t, b] = total[b * seqs : (b + 1) * seqs, :].astype(BF16)
        for d in range(blocks(t) // CORES):
            for r in range(CORES):
                if isinstance(t, int) and t == half and r == 0:
                    q_in[gx] = q_send[half, c]
                else:
                    q_copy(t, d, r).start()

    for j in range(IN_CHUNKS):
        for d in range(2):
            ring(d, 0, j).start()
    for j in range(IN_CHUNKS):
        ref = own_slot.at[:, piece(j)]
        remote(ref, ref, pair_send_sem.at[0, half], pair_sem.at[0, half], pair).start()
    for load in loads[2:]:
        load.start()
    wo_copy = remote(w_out.at[:, half_cols(other)], wo.at[c], wo_send_sem, wo_sem, pair)
    wo_copy.start()

    def gather_step(s):
        known = isinstance(s, int)
        before = half if known and s == 0 else s - 1
        for j in range(IN_CHUNKS):
            for d in range(2):
                if not known or travels(d, s, j):
                    ring(d, s, j).wait_recv()
                    if not known or (s < half - 1 and travels(d, s + 1, j)):
                        ring(d, s + 1, j).start()
                    to_pair(d, s, j).start()
            if known and s == 0 and j == 0:
                loads[1].wait()
            dot_piece(before, j)
        send_parts(before)
        if not known or s > 0:
            send_queries(half if known and s == 1 else s - 2)

    gather_step(0)
    gather_step(1)

    @pl.loop(2, half - 2)
    def _(s):
        gather_step(s)

    for s in range(max(half - 2, 2), half):
        gather_step(s)
    for j in range(IN_CHUNKS):
        dot_piece(half - 1, j)
    send_parts(half - 1)
    send_queries(half - 2)
    send_queries(half - 1)

    for load in loads[3:]:
        load.wait()

    @pl.loop(1, nz * CORES)
    def _(k):
        ref = q_in.at[lax.rem(gx + k, nz * CORES)]
        remote(ref, ref, q_send_sem, q_sem.at[lax.rem(gx + k, nz * CORES)], pair).wait_recv()

    q_wide[...] = q_in[...].reshape(nz, CORES, seqs, feats).astype(F32)
    heads = CORES * feats // hd
    for i in range(seqs):
        rows = jnp.concatenate([q_wide[:, core, i, :] for core in range(CORES)], axis=1)
        query = jnp.concatenate([rows[:, h * hd : (h + 1) * hd] for h in range(heads)], axis=0).astype(BF16)
        scores = lax.dot_general(query, k_buf[i], (((1,), (1,)), ((), ())), preferred_element_type=F32)
        scores = scores * F32(hd**-0.5)
        live = lax.broadcasted_iota(jnp.int32, scores.shape, 1) < lengths[i]
        scores = jnp.where(live, scores, F32(-1e30))
        expo = jnp.where(live, jnp.exp(scores - jnp.max(scores, axis=1, keepdims=True)), F32(0.0))
        probs = (expo / jnp.sum(expo, axis=1, keepdims=True)).astype(BF16)
        mixed = jnp.dot(probs, v_buf[i], preferred_element_type=F32)
        wide = jnp.concatenate([mixed[h * nz : (h + 1) * nz, :] for h in range(heads)], axis=1)
        for core in range(CORES):
            att_wide[:, core, i, :] = wide[:, core * feats : (core + 1) * feats]
    att_send[...] = att_wide[...].astype(BF16)

    def att_copy(v, r):
        core = lax.rem(c + r, CORES)
        chip = z - source_offset(v, half)
        return remote(
            att_send.at[lax.rem(chip + nz, nz), core], att_in.at[x, v, c], att_send_sem, att_sem.at[v, c], at_z(chip, core)
        )

    for v in [*range(1, nz), 0]:
        for r in range(CORES):
            if v == 0 and r == 0:
                att_in[x, v, c] = att_send[z, c]
            else:
                att_copy(v, r).start()

    batches = nz // PER_BATCH

    def batch(b):
        return pl.ds(b * PER_BATCH, PER_BATCH)

    def rows_copy(b, k):
        ref = att_in.at[x, batch(b)]
        return remote(ref, ref, rows_send_sem.at[b, k - 1], rows_sem.at[b, k - 1], at_x(k))

    def swap_copy(b):
        ref = att.at[c, batch(b)]
        return remote(ref, ref, swap_send_sem.at[b], swap_sem.at[b], pair)

    def pass_on(b):
        for k in range(1, nx):
            rows_copy(b, k).wait_recv()
        for n in range(PER_BATCH):
            for core in range(CORES):
                v = b * PER_BATCH + n
                att[c, v, core] = jnp.concatenate(
                    [att_in[g, v, core].astype(F32) for g in range(nx)], axis=0
                ).astype(BF16)
        swap_copy(b).start()

    for b in range(batches):
        for v in range(b * PER_BATCH, (b + 1) * PER_BATCH):
            for r in range(CORES):
                core = lax.rem(c + r, CORES)
                if v > 0 or r > 0:
                    ref = att_in.at[x, v, core]
                    remote(ref, ref, att_send_sem, att_sem.at[v, core], pair).wait_recv()
        for k in range(1, nx):
            rows_copy(b, k).start()
    pass_on(0)
    loads[2].wait()
    wo_copy.wait_recv()

    def out_piece(j):
        return pl.ds(j * out_cols, out_cols)

    def projected(v, count, j):
        lhs = jnp.concatenate(
            [att[f, pl.ds(v, count)].reshape(count * CORES * block, feats) for f in range(CORES)], axis=1
        )
        rhs = wo[:, :, j * out_cols : (j + 1) * out_cols].reshape(CORES * feats, out_cols)
        return jnp.dot(lhs, rhs, preferred_element_type=F32)

    def sums_copy(d, s, j):
        return remote(
            sums.at[d, s, :, out_piece(j)],
            sums_in.at[d, s, :, out_piece(j)],
            sums_send_sem.at[d, s],
            sums_sem.at[d, s, j],
            side[d],
        )

    def starts(d, j):
        return (j < (OUT_CHUNKS + 1) // 2) == (d == 0)

    tall = CORES * block

    def out_step(s):
        known = isinstance(s, int)
        for j in range(OUT_CHUNKS):
            span = slice(j * out_cols, (j + 1) * out_cols)
            if known and s == 0:
                d = 0 if starts(0, j) else 1
                sums[d, 0, :, span] = projected(1, 1, j).astype(BF16)
                sums_copy(d, 0, j).start()
                continue
            both = projected(2 * s, 2, j)
            for d in range(2):
                term = both[d * tall : (d + 1) * tall]
                if not known or s > 1 or starts(d, j):
                    sums_copy(d, s - 1, j).wait_recv()
                    term = term + sums_in[d, s - 1, :, span].astype(F32)
                sums[d, s, :, span] = term.astype(BF16)
                sums_copy(d, s, j).start()

    pass_on(1)
    swap_copy(0).wait_recv()
    out_step(0)
    out_step(1)

    @pl.loop(1, batches - 1)
    def _(b):
        pass_on(b + 1)
        swap_copy(b).wait_recv()
        out_step(2 * b)
        out_step(2 * b + 1)

    swap_copy(batches - 1).wait_recv()

    @pl.loop(half - 2, half)
    def _(s):
        out_step(s)

    def last_copy(j):
        own = pl.ds(pl.multiple_of(c * own_cols + j * out_cols, 128), out_cols)
        return remote(
            last.at[other, :, out_piece(j)], out.at[:, own], last_send_sem.at[j], last_sem.at[j], pair
        )

    for j in range(OUT_CHUNKS):
        span = slice(j * out_cols, (j + 1) * out_cols)
        term = projected(0, 1, j)
        for d in range(2):
            sums_copy(d, half - 1, j).wait_recv()
            term = term + sums_in[d, half - 1, :, span].astype(F32)
        for core in range(CORES):
            last[core, :, span] = term[core * block : (core + 1) * block].astype(BF16)
        last_copy(j).start()
    out[:, half_cols(c)] = last[c]
    for j in range(OUT_CHUNKS):
        last_copy(j).wait_recv()

    def left(ref, sem, recv_sem, device):
        remote(ref, ref, sem, recv_sem, device).wait_send()

    @pl.loop(0, half - 1)
    def _(t):
        for d in range(2):
            left(gathered.at[0, c], pair_send_sem.at[d, t], pair_sem.at[d, t], pair)
            left(gathered.at[0, c], ring_send_sem.at[d, t], ring_sem.at[d, t, 0], side[d])
        for k in range(1, nx):
            part_copy(t, k).wait_send()

    for t in (half - 1, half):
        left(gathered.at[0, c], pair_send_sem.at[0, t], pair_sem.at[0, t], pair)
        for k in range(1, nx):
            part_copy(t, k).wait_send()

    @pl.loop(1, half)
    def _(s):
        for d in range(2):
            left(sums.at[d, s], sums_send_sem.at[d, s], sums_sem.at[d, s, 0], side[d])

    for d in range(2):
        left(
            gathered.at[0, c, :, pl.ds(0, width // 2)], ring_send_sem.at[d, half - 1], ring_sem.at[d, half - 1, 0], side[d]
        )
        first = out_cols * sum(starts(d, j) for j in range(OUT_CHUNKS))
        left(sums.at[d, 0, :, pl.ds(0, first)], sums_send_sem.at[d, 0], sums_sem.at[d, 0, 0], side[d])
    ref = q_in.at[pl.ds(0, nz * CORES - 1)]
    left(ref, q_send_sem, q_sem.at[0], pair)
    left(ref, att_send_sem, att_sem.at[0, 0], pair)
    for b in range(batches):
        swap_copy(b).wait_send()
        for k in range(1, nx):
            rows_copy(b, k).wait_send()
    wo_copy.wait_send()
    for j in range(OUT_CHUNKS):
        last_copy(j).wait_send()


def solution(mesh):
    nz = mesh.shape["gx"] // CORES
    nx = mesh.shape["gy"]
    half = nz // 2

    def body(hidden_in, w_query, w_out, cache_keys, cache_values, lengths):
        block, width = hidden_in.shape
        feats = w_query.shape[1]
        seqs, slots, hd = cache_keys.shape
        own_cols = width // CORES
        dma = pltpu.SemaphoreType.DMA
        hbm = pl.BlockSpec(memory_space=pltpu.HBM)
        return pl.pallas_call(
            functools.partial(kernel, nz, nx),
            out_shape=jax.ShapeDtypeStruct((block, width), BF16),
            in_specs=[pl.BlockSpec(memory_space=pltpu.SMEM)] + [hbm] * 5,
            out_specs=pl.BlockSpec(memory_space=pltpu.VMEM),
            scratch_shapes=[
                pltpu.VMEM((half + 1, 2 * CORES, block, width), BF16),
                pltpu.VMEM(w_query.shape, BF16),
                pltpu.VMEM((CORES, feats, own_cols), BF16),
                pltpu.VMEM(cache_keys.shape, BF16),
                pltpu.VMEM(cache_values.shape, BF16),
                pltpu.VMEM((2 * CORES * block, feats), F32),
                pltpu.VMEM((half + 1, nx, 2 * CORES * seqs, feats), F32),
                pltpu.VMEM((half + 1, nx - 1, 2 * CORES * seqs, feats), F32),
                pltpu.VMEM((half + 1, 2 * CORES, seqs, feats), BF16),
                pltpu.VMEM((nz * CORES, seqs, feats), BF16),
                pltpu.VMEM((nz, CORES, seqs, feats), F32),
                pltpu.VMEM((nz, CORES, seqs, feats), F32),
                pltpu.VMEM((nz, CORES, seqs, feats), BF16),
                pltpu.VMEM((nx, nz, CORES, seqs, feats), BF16),
                pltpu.VMEM((CORES, nz, CORES, block, feats), BF16),
                pltpu.VMEM((2, half, CORES * block, own_cols), BF16),
                pltpu.VMEM((2, half, CORES * block, own_cols), BF16),
                pltpu.VMEM((CORES, block, own_cols), BF16),
                dma((5,)),
                dma((2, half)),
                dma((2, half, IN_CHUNKS)),
                dma((2, half + 1)),
                dma((2, half + 1)),
                dma((half + 1, nx - 1)),
                dma((half + 1, nx - 1)),
                dma(()),
                dma((nz * CORES,)),
                dma(()),
                dma((nz, CORES)),
                dma((nz // PER_BATCH, nx - 1)),
                dma((nz // PER_BATCH, nx - 1)),
                dma((nz // PER_BATCH,)),
                dma((nz // PER_BATCH,)),
                dma(()),
                dma(()),
                dma((2, half)),
                dma((2, half, OUT_CHUNKS)),
                dma((OUT_CHUNKS,)),
                dma((OUT_CHUNKS,)),
            ],
            compiler_params=pltpu.CompilerParams(
                collective_id=0, has_side_effects=True, vmem_limit_bytes=60 * 2**20
            ),
            name="decode_step",
        )(lengths, hidden_in, w_query, w_out, cache_keys, cache_values)

    return jax.shard_map(
        body,
        mesh=mesh,
        in_specs=(
            P(("groups", "gx"), "gy"),
            P("gy", "gx"),
            P("gx", "gy"),
            P(("groups", "gx", "gy"), None, None),
            P(("groups", "gx", "gy"), None, None),
            P(("groups", "gx", "gy")),
        ),
        out_specs=P(("groups", "gx"), "gy"),
        check_vma=False,
    )
```

```python
import functools

import jax
import jax.numpy as jnp
from jax import lax
from jax.experimental import pallas as pl
from jax.experimental.pallas import tpu as pltpu
from jax.sharding import PartitionSpec as P

MESH = pl.DeviceIdType.MESH
CORES = 2
IN_CHUNKS = 6
OUT_CHUNKS = 9
PER_BATCH = 4
F32 = jnp.float32
BF16 = jnp.bfloat16


def source_offset(v, half):
    return half - (v + 1) // 2 if v % 2 else half + v // 2


def kernel(
    nz,
    nx,
    lengths,
    hidden,
    w_query,
    w_out,
    keys,
    values,
    out,
    gathered,
    wq,
    wo,
    k_buf,
    v_buf,
    acc,
    part,
    part_in,
    q_send,
    q_in,
    q_wide,
    att_wide,
    att_send,
    att_in,
    att,
    sums,
    sums_in,
    last,
    local_sem,
    ring_send_sem,
    ring_sem,
    pair_send_sem,
    pair_sem,
    part_send_sem,
    part_sem,
    q_send_sem,
    q_sem,
    att_send_sem,
    att_sem,
    rows_send_sem,
    rows_sem,
    swap_send_sem,
    swap_sem,
    wo_send_sem,
    wo_sem,
    sums_send_sem,
    sums_sem,
    last_send_sem,
    last_sem,
):
    half = nz // 2
    gx = lax.axis_index("gx")
    x = lax.axis_index("gy")
    z = gx // CORES
    c = gx % CORES
    other = 1 - c
    seqs, slots, hd = k_buf.shape
    width = hidden.shape[1]
    cols = width // IN_CHUNKS
    own_cols = width // CORES
    out_cols = own_cols // OUT_CHUNKS
    feats = w_query.shape[1]
    block = nx * seqs

    def at_z(chip, core):
        return {"gx": lax.rem(chip + 2 * nz, nz) * CORES + core}

    def at_x(offset):
        return {"gy": lax.rem(x + offset, nx)}

    side = (at_z(z + 1, c), at_z(z - 1, c))
    pair = {"gx": z * CORES + other}

    def remote(src, dst, send_sem, recv_sem, device):
        return pltpu.make_async_remote_copy(
            src_ref=src, dst_ref=dst, send_sem=send_sem, recv_sem=recv_sem, device_id=device, device_id_type=MESH
        )

    def half_cols(core):
        return pl.ds(pl.multiple_of(core * own_cols, 128), own_cols)

    own_slot = gathered.at[half, c]
    loads = [
        pltpu.make_async_copy(hidden, own_slot, local_sem.at[0]),
        pltpu.make_async_copy(w_query, wq, local_sem.at[1]),
        pltpu.make_async_copy(w_out.at[:, half_cols(c)], wo.at[c], local_sem.at[2]),
        pltpu.make_async_copy(keys, k_buf, local_sem.at[3]),
        pltpu.make_async_copy(values, v_buf, local_sem.at[4]),
    ]
    loads[0].start()
    loads[1].start()

    barrier = pltpu.get_barrier_semaphore()
    greeted = [*side, pair] + [at_x(k) for k in range(1, nx)]
    for device in greeted:
        pl.semaphore_signal(barrier, inc=1, device_id=device, device_id_type=MESH)
    pl.semaphore_wait(barrier, len(greeted))
    loads[0].wait()

    def piece(j):
        return pl.ds(j * cols, cols)

    def home(s, d):
        return 0 if isinstance(s, int) and s == half - 1 else d

    def ring(d, s, j):
        src = own_slot if isinstance(s, int) and s == 0 else gathered.at[s - 1, CORES * d + c]
        dst = gathered.at[s, CORES * home(s, d) + c]
        return remote(src.at[:, piece(j)], dst.at[:, piece(j)], ring_send_sem.at[d, s], ring_sem.at[d, s, j], side[d])

    def to_pair(d, s, j):
        ref = gathered.at[s, CORES * home(s, d) + c, :, piece(j)]
        return remote(ref, ref, pair_send_sem.at[home(s, d), s], pair_sem.at[home(s, d), s], pair)

    def travels(d, s, j):
        return s < half - 1 or (j < IN_CHUNKS // 2) == (d == 0)

    def blocks(t):
        return CORES if isinstance(t, int) and t >= half - 1 else 2 * CORES

    def dot_piece(t, j):
        if j == 0:
            for d in range(blocks(t) // CORES):
                ref = gathered.at[t, CORES * d + other]
                remote(ref, ref, pair_send_sem.at[d, t], pair_sem.at[d, t], pair).wait_recv()
        tall = blocks(t) * block
        lhs = gathered[t, : blocks(t), :, j * cols : (j + 1) * cols].reshape(tall, cols)
        term = jnp.dot(lhs, wq[j * cols : (j + 1) * cols, :], preferred_element_type=F32)
        if j == 0:
            acc[:tall] = term
        else:
            acc[:tall] += term

    def part_copy(t, k):
        rows = pl.ds(0, blocks(t) * seqs)
        return remote(
            part.at[t, lax.rem(x + k, nx), rows],
            part_in.at[t, k - 1, rows],
            part_send_sem.at[t, k - 1],
            part_sem.at[t, k - 1],
            at_x(k),
        )

    def send_parts(t):
        for g in range(nx):
            part[t, g, : blocks(t) * seqs] = jnp.concatenate(
                [acc[b * block + g * seqs : b * block + (g + 1) * seqs, :] for b in range(blocks(t))], axis=0
            )
        for k in range(1, nx):
            part_copy(t, k).start()

    def q_copy(t, d, r):
        core = lax.rem(c + r, CORES)
        if isinstance(t, int) and t >= half - 1:
            chip = z if t == half else z + half
        else:
            chip = z - 1 - t if d == 0 else z + 1 + t
        return remote(q_send.at[t, CORES * d + core], q_in.at[gx], q_send_sem, q_sem.at[gx], at_z(chip, core))

    def send_queries(t):
        rows = blocks(t) * seqs
        total = part[t, x, :rows]
        for k in range(1, nx):
            part_copy(t, k).wait_recv()
            total = total + part_in[t, k - 1, :rows]
        for b in range(blocks(t)):
            q_send[t, b] = total[b * seqs : (b + 1) * seqs, :].astype(BF16)
        for d in range(blocks(t) // CORES):
            for r in range(CORES):
                if isinstance(t, int) and t == half and r == 0:
                    q_in[gx] = q_send[half, c]
                else:
                    q_copy(t, d, r).start()

    for j in range(IN_CHUNKS):
        for d in range(2):
            ring(d, 0, j).start()
    for j in range(IN_CHUNKS):
        ref = own_slot.at[:, piece(j)]
        remote(ref, ref, pair_send_sem.at[0, half], pair_sem.at[0, half], pair).start()
    for load in loads[2:]:
        load.start()
    wo_copy = remote(w_out.at[:, half_cols(other)], wo.at[c], wo_send_sem, wo_sem, pair)
    wo_copy.start()

    def gather_step(s):
        known = isinstance(s, int)
        before = half if known and s == 0 else s - 1
        for j in range(IN_CHUNKS):
            for d in range(2):
                if not known or travels(d, s, j):
                    ring(d, s, j).wait_recv()
                    if not known or (s < half - 1 and travels(d, s + 1, j)):
                        ring(d, s + 1, j).start()
                    to_pair(d, s, j).start()
            if known and s == 0 and j == 0:
                loads[1].wait()
            dot_piece(before, j)
        send_parts(before)
        if not known or s > 0:
            send_queries(half if known and s == 1 else s - 2)

    gather_step(0)
    gather_step(1)

    @pl.loop(2, half - 2)
    def _(s):
        gather_step(s)

    for s in range(max(half - 2, 2), half):
        gather_step(s)
    for j in range(IN_CHUNKS):
        dot_piece(half - 1, j)
    send_parts(half - 1)
    send_queries(half - 2)
    send_queries(half - 1)

    for load in loads[3:]:
        load.wait()

    @pl.loop(1, nz * CORES)
    def _(k):
        ref = q_in.at[lax.rem(gx + k, nz * CORES)]
        remote(ref, ref, q_send_sem, q_sem.at[lax.rem(gx + k, nz * CORES)], pair).wait_recv()

    q_wide[...] = q_in[...].reshape(nz, CORES, seqs, feats).astype(F32)
    heads = CORES * feats // hd

    def scores_of(i):
        rows = jnp.concatenate([q_wide[:, core, i, :] for core in range(CORES)], axis=1)
        query = jnp.concatenate([rows[:, h * hd : (h + 1) * hd] for h in range(heads)], axis=0).astype(BF16)
        return lax.dot_general(query, k_buf[i], (((1,), (1,)), ((), ())), preferred_element_type=F32)

    def probs_of(i, scores):
        scores = scores * F32(hd**-0.5)
        live = lax.broadcasted_iota(jnp.int32, scores.shape, 1) < lengths[i]
        scores = jnp.where(live, scores, F32(-1e30))
        expo = jnp.where(live, jnp.exp(scores - jnp.max(scores, axis=1, keepdims=True)), F32(0.0))
        return (expo / jnp.sum(expo, axis=1, keepdims=True)).astype(BF16)

    scores = [scores_of(i) for i in range(seqs)]
    probs = [probs_of(i, scores[i]) for i in range(seqs)]
    mixed = [jnp.dot(probs[i], v_buf[i], preferred_element_type=F32) for i in range(seqs)]
    for i in range(seqs):
        wide = jnp.concatenate([mixed[i][h * nz : (h + 1) * nz, :] for h in range(heads)], axis=1)
        for core in range(CORES):
            att_wide[:, core, i, :] = wide[:, core * feats : (core + 1) * feats]
    att_send[...] = att_wide[...].astype(BF16)

    def att_copy(v, r):
        core = lax.rem(c + r, CORES)
        chip = z - source_offset(v, half)
        return remote(
            att_send.at[lax.rem(chip + nz, nz), core], att_in.at[x, v, c], att_send_sem, att_sem.at[v, c], at_z(chip, core)
        )

    for v in range(nz):
        for r in range(CORES):
            if v == nz - 1 and r == 0:
                att_in[x, v, c] = att_send[z, c]
            else:
                att_copy(v, r).start()

    own_batch = nz // PER_BATCH + 1

    def batch(b):
        known = isinstance(b, int)
        if known and b in (0, own_batch):
            return (0 if b == 0 else nz - 1), 1
        return (1, 2) if known and b == 1 else (PER_BATCH * b - 5, PER_BATCH)

    def rows_copy(b, k):
        ref = att_in.at[x, pl.ds(*batch(b))]
        return remote(ref, ref, rows_send_sem.at[b, k - 1], rows_sem.at[b, k - 1], at_x(k))

    def swap_copy(b):
        ref = att.at[c, pl.ds(*batch(b))]
        return remote(ref, ref, swap_send_sem.at[b], swap_sem.at[b], pair)

    def pass_on(b):
        for k in range(1, nx):
            rows_copy(b, k).wait_recv()
        start, count = batch(b)
        for n in range(count):
            for core in range(CORES):
                v = start + n
                att[c, v, core] = jnp.concatenate(
                    [att_in[g, v, core].astype(F32) for g in range(nx)], axis=0
                ).astype(BF16)
        swap_copy(b).start()

    for b in range(own_batch + 1):
        start, count = batch(b)
        for v in range(start, start + count):
            for r in range(CORES):
                core = lax.rem(c + r, CORES)
                if v < nz - 1 or r > 0:
                    ref = att_in.at[x, v, core]
                    remote(ref, ref, att_send_sem, att_sem.at[v, core], pair).wait_recv()
        for k in range(1, nx):
            rows_copy(b, k).start()
    pass_on(0)
    loads[2].wait()
    wo_copy.wait_recv()

    def out_piece(j):
        return pl.ds(j * out_cols, out_cols)

    def projected(v, count, j):
        lhs = jnp.concatenate(
            [att[f, pl.ds(v, count)].reshape(count * CORES * block, feats) for f in range(CORES)], axis=1
        )
        rhs = wo[:, :, j * out_cols : (j + 1) * out_cols].reshape(CORES * feats, out_cols)
        return jnp.dot(lhs, rhs, preferred_element_type=F32)

    def sums_copy(d, s, j):
        return remote(
            sums.at[d, s, :, out_piece(j)],
            sums_in.at[d, s, :, out_piece(j)],
            sums_send_sem.at[d, s],
            sums_sem.at[d, s, j],
            side[d],
        )

    def starts(d, j):
        return (j < (OUT_CHUNKS + 1) // 2) == (d == 0)

    tall = CORES * block

    def out_step(s):
        known = isinstance(s, int)
        for j in range(OUT_CHUNKS):
            span = slice(j * out_cols, (j + 1) * out_cols)
            if known and s == 0:
                d = 0 if starts(0, j) else 1
                sums[d, 0, :, span] = projected(0, 1, j).astype(BF16)
                sums_copy(d, 0, j).start()
                continue
            both = projected(2 * s - 1, 2, j)
            for d in range(2):
                term = both[d * tall : (d + 1) * tall]
                if not known or s > 1 or starts(d, j):
                    sums_copy(d, s - 1, j).wait_recv()
                    term = term + sums_in[d, s - 1, :, span].astype(F32)
                sums[d, s, :, span] = term.astype(BF16)
                sums_copy(d, s, j).start()

    pass_on(1)
    swap_copy(0).wait_recv()
    out_step(0)
    pass_on(2)
    swap_copy(1).wait_recv()
    out_step(1)

    @pl.loop(2, own_batch - 1)
    def _(b):
        pass_on(b + 1)
        swap_copy(b).wait_recv()
        out_step(2 * b - 2)
        out_step(2 * b - 1)

    pass_on(own_batch)
    swap_copy(own_batch - 1).wait_recv()

    @pl.loop(half - 2, half)
    def _(s):
        out_step(s)

    swap_copy(own_batch).wait_recv()

    def last_copy(j):
        own = pl.ds(pl.multiple_of(c * own_cols + j * out_cols, 128), out_cols)
        return remote(
            last.at[other, :, out_piece(j)], out.at[:, own], last_send_sem.at[j], last_sem.at[j], pair
        )

    for j in range(OUT_CHUNKS):
        span = slice(j * out_cols, (j + 1) * out_cols)
        term = projected(nz - 1, 1, j)
        for d in range(2):
            sums_copy(d, half - 1, j).wait_recv()
            term = term + sums_in[d, half - 1, :, span].astype(F32)
        for core in range(CORES):
            last[core, :, span] = term[core * block : (core + 1) * block].astype(BF16)
        last_copy(j).start()
    out[:, half_cols(c)] = last[c]
    for j in range(OUT_CHUNKS):
        last_copy(j).wait_recv()

    def left(ref, sem, recv_sem, device):
        remote(ref, ref, sem, recv_sem, device).wait_send()

    @pl.loop(0, half - 1)
    def _(t):
        for d in range(2):
            left(gathered.at[0, c], pair_send_sem.at[d, t], pair_sem.at[d, t], pair)
            left(gathered.at[0, c], ring_send_sem.at[d, t], ring_sem.at[d, t, 0], side[d])
        for k in range(1, nx):
            part_copy(t, k).wait_send()

    for t in (half - 1, half):
        left(gathered.at[0, c], pair_send_sem.at[0, t], pair_sem.at[0, t], pair)
        for k in range(1, nx):
            part_copy(t, k).wait_send()

    @pl.loop(1, half)
    def _(s):
        for d in range(2):
            left(sums.at[d, s], sums_send_sem.at[d, s], sums_sem.at[d, s, 0], side[d])

    for d in range(2):
        left(
            gathered.at[0, c, :, pl.ds(0, width // 2)], ring_send_sem.at[d, half - 1], ring_sem.at[d, half - 1, 0], side[d]
        )
        first = out_cols * sum(starts(d, j) for j in range(OUT_CHUNKS))
        left(sums.at[d, 0, :, pl.ds(0, first)], sums_send_sem.at[d, 0], sums_sem.at[d, 0, 0], side[d])
    ref = q_in.at[pl.ds(0, nz * CORES - 1)]
    left(ref, q_send_sem, q_sem.at[0], pair)
    left(ref, att_send_sem, att_sem.at[0, 0], pair)
    for b in range(own_batch + 1):
        swap_copy(b).wait_send()
        for k in range(1, nx):
            rows_copy(b, k).wait_send()
    wo_copy.wait_send()
    for j in range(OUT_CHUNKS):
        last_copy(j).wait_send()


def solution(mesh):
    nz = mesh.shape["gx"] // CORES
    nx = mesh.shape["gy"]
    half = nz // 2

    def body(hidden_in, w_query, w_out, cache_keys, cache_values, lengths):
        block, width = hidden_in.shape
        feats = w_query.shape[1]
        seqs, slots, hd = cache_keys.shape
        own_cols = width // CORES
        dma = pltpu.SemaphoreType.DMA
        hbm = pl.BlockSpec(memory_space=pltpu.HBM)
        return pl.pallas_call(
            functools.partial(kernel, nz, nx),
            out_shape=jax.ShapeDtypeStruct((block, width), BF16),
            in_specs=[pl.BlockSpec(memory_space=pltpu.SMEM)] + [hbm] * 5,
            out_specs=pl.BlockSpec(memory_space=pltpu.VMEM),
            scratch_shapes=[
                pltpu.VMEM((half + 1, 2 * CORES, block, width), BF16),
                pltpu.VMEM(w_query.shape, BF16),
                pltpu.VMEM((CORES, feats, own_cols), BF16),
                pltpu.VMEM(cache_keys.shape, BF16),
                pltpu.VMEM(cache_values.shape, BF16),
                pltpu.VMEM((2 * CORES * block, feats), F32),
                pltpu.VMEM((half + 1, nx, 2 * CORES * seqs, feats), F32),
                pltpu.VMEM((half + 1, nx - 1, 2 * CORES * seqs, feats), F32),
                pltpu.VMEM((half + 1, 2 * CORES, seqs, feats), BF16),
                pltpu.VMEM((nz * CORES, seqs, feats), BF16),
                pltpu.VMEM((nz, CORES, seqs, feats), F32),
                pltpu.VMEM((nz, CORES, seqs, feats), F32),
                pltpu.VMEM((nz, CORES, seqs, feats), BF16),
                pltpu.VMEM((nx, nz, CORES, seqs, feats), BF16),
                pltpu.VMEM((CORES, nz, CORES, block, feats), BF16),
                pltpu.VMEM((2, half, CORES * block, own_cols), BF16),
                pltpu.VMEM((2, half, CORES * block, own_cols), BF16),
                pltpu.VMEM((CORES, block, own_cols), BF16),
                dma((5,)),
                dma((2, half)),
                dma((2, half, IN_CHUNKS)),
                dma((2, half + 1)),
                dma((2, half + 1)),
                dma((half + 1, nx - 1)),
                dma((half + 1, nx - 1)),
                dma(()),
                dma((nz * CORES,)),
                dma(()),
                dma((nz, CORES)),
                dma((nz // PER_BATCH + 2, nx - 1)),
                dma((nz // PER_BATCH + 2, nx - 1)),
                dma((nz // PER_BATCH + 2,)),
                dma((nz // PER_BATCH + 2,)),
                dma(()),
                dma(()),
                dma((2, half)),
                dma((2, half, OUT_CHUNKS)),
                dma((OUT_CHUNKS,)),
                dma((OUT_CHUNKS,)),
            ],
            compiler_params=pltpu.CompilerParams(
                collective_id=0, has_side_effects=True, vmem_limit_bytes=52 * 2**20
            ),
            name="decode_step",
        )(lengths, hidden_in, w_query, w_out, cache_keys, cache_values)

    return jax.shard_map(
        body,
        mesh=mesh,
        in_specs=(
            P(("groups", "gx"), "gy"),
            P("gy", "gx"),
            P("gx", "gy"),
            P(("groups", "gx", "gy"), None, None),
            P(("groups", "gx", "gy"), None, None),
            P(("groups", "gx", "gy")),
        ),
        out_specs=P(("groups", "gx"), "gy"),
        check_vma=False,
    )
```

```python
import functools

import jax
import jax.numpy as jnp
from jax import lax
from jax.experimental import pallas as pl
from jax.experimental.pallas import tpu as pltpu
from jax.sharding import PartitionSpec as P

MESH = pl.DeviceIdType.MESH
CORES = 2
IN_CHUNKS = 6
OUT_CHUNKS = 9
PER_BATCH = 4
F32 = jnp.float32
BF16 = jnp.bfloat16


def source_offset(v, half):
    return half - (v + 1) // 2 if v % 2 else half + v // 2


def kernel(
    nz,
    nx,
    lengths,
    hidden,
    w_query,
    w_out,
    keys,
    values,
    out,
    gathered,
    wq,
    wo,
    k_buf,
    v_buf,
    acc,
    part,
    part_in,
    q_send,
    q_in,
    q_wide,
    att_wide,
    att_send,
    att_in,
    att,
    sums,
    sums_in,
    last,
    local_sem,
    ring_send_sem,
    ring_sem,
    pair_send_sem,
    pair_sem,
    part_send_sem,
    part_sem,
    q_send_sem,
    q_sem,
    att_send_sem,
    att_sem,
    rows_send_sem,
    rows_sem,
    swap_send_sem,
    swap_sem,
    wo_send_sem,
    wo_sem,
    sums_send_sem,
    sums_sem,
    last_send_sem,
    last_sem,
):
    half = nz // 2
    gx = lax.axis_index("gx")
    x = lax.axis_index("gy")
    z = gx // CORES
    c = gx % CORES
    other = 1 - c
    seqs, slots, hd = k_buf.shape
    width = hidden.shape[1]
    cols = width // IN_CHUNKS
    own_cols = width // CORES
    out_cols = own_cols // OUT_CHUNKS
    feats = w_query.shape[1]
    block = nx * seqs

    def at_z(chip, core):
        return {"gx": lax.rem(chip + 2 * nz, nz) * CORES + core}

    def at_x(offset):
        return {"gy": lax.rem(x + offset, nx)}

    side = (at_z(z + 1, c), at_z(z - 1, c))
    pair = {"gx": z * CORES + other}

    def remote(src, dst, send_sem, recv_sem, device):
        return pltpu.make_async_remote_copy(
            src_ref=src, dst_ref=dst, send_sem=send_sem, recv_sem=recv_sem, device_id=device, device_id_type=MESH
        )

    def half_cols(core):
        return pl.ds(pl.multiple_of(core * own_cols, 128), own_cols)

    own_slot = gathered.at[half, c]
    loads = [
        pltpu.make_async_copy(hidden, own_slot, local_sem.at[0]),
        pltpu.make_async_copy(w_query, wq, local_sem.at[1]),
        pltpu.make_async_copy(w_out.at[:, half_cols(c)], wo.at[c], local_sem.at[2]),
        pltpu.make_async_copy(keys, k_buf, local_sem.at[3]),
        pltpu.make_async_copy(values, v_buf, local_sem.at[4]),
    ]
    loads[0].start()
    loads[1].start()

    barrier = pltpu.get_barrier_semaphore()
    greeted = [*side, pair] + [at_x(k) for k in range(1, nx)]
    for device in greeted:
        pl.semaphore_signal(barrier, inc=1, device_id=device, device_id_type=MESH)
    pl.semaphore_wait(barrier, len(greeted))
    loads[0].wait()

    def piece(j):
        return pl.ds(j * cols, cols)

    def home(s, d):
        return 0 if isinstance(s, int) and s == half - 1 else d

    def ring(d, s, j):
        src = own_slot if isinstance(s, int) and s == 0 else gathered.at[s - 1, CORES * d + c]
        dst = gathered.at[s, CORES * home(s, d) + c]
        return remote(src.at[:, piece(j)], dst.at[:, piece(j)], ring_send_sem.at[d, s], ring_sem.at[d, s, j], side[d])

    def to_pair(d, s, j):
        ref = gathered.at[s, CORES * home(s, d) + c, :, piece(j)]
        return remote(ref, ref, pair_send_sem.at[home(s, d), s], pair_sem.at[home(s, d), s], pair)

    def travels(d, s, j):
        return s < half - 1 or (j < IN_CHUNKS // 2) == (d == 0)

    def blocks(t):
        return CORES if isinstance(t, int) and t >= half - 1 else 2 * CORES

    def dot_piece(t, j):
        if j == 0:
            for d in range(blocks(t) // CORES):
                ref = gathered.at[t, CORES * d + other]
                remote(ref, ref, pair_send_sem.at[d, t], pair_sem.at[d, t], pair).wait_recv()
        tall = blocks(t) * block
        lhs = gathered[t, : blocks(t), :, j * cols : (j + 1) * cols].reshape(tall, cols)
        term = jnp.dot(lhs, wq[j * cols : (j + 1) * cols, :], preferred_element_type=F32)
        if j == 0:
            acc[:tall] = term
        else:
            acc[:tall] += term

    def part_copy(t, k):
        rows = pl.ds(0, blocks(t) * seqs)
        return remote(
            part.at[t, lax.rem(x + k, nx), rows],
            part_in.at[t, k - 1, rows],
            part_send_sem.at[t, k - 1],
            part_sem.at[t, k - 1],
            at_x(k),
        )

    def send_parts(t):
        for g in range(nx):
            part[t, g, : blocks(t) * seqs] = jnp.concatenate(
                [acc[b * block + g * seqs : b * block + (g + 1) * seqs, :] for b in range(blocks(t))], axis=0
            )
        for k in range(1, nx):
            part_copy(t, k).start()

    def q_copy(t, d, r):
        core = lax.rem(c + r, CORES)
        if isinstance(t, int) and t >= half - 1:
            chip = z if t == half else z + half
        else:
            chip = z - 1 - t if d == 0 else z + 1 + t
        slot = 2 * (half - 1 - t) - 1 + d
        if isinstance(t, int) and t >= half - 1:
            slot = nz - 1 if t == half else 0
        return remote(
            q_send.at[t, CORES * d + core], q_in.at[slot, c], q_send_sem.at[r], q_sem.at[slot, c], at_z(chip, core)
        )

    def send_queries(t):
        rows = blocks(t) * seqs
        total = part[t, x, :rows]
        for k in range(1, nx):
            part_copy(t, k).wait_recv()
            total = total + part_in[t, k - 1, :rows]
        for b in range(blocks(t)):
            q_send[t, b] = total[b * seqs : (b + 1) * seqs, :].astype(BF16)
        for d in range(blocks(t) // CORES):
            for r in range(CORES):
                if isinstance(t, int) and t == half and r == 0:
                    q_in[nz - 1, c] = q_send[half, c]
                else:
                    q_copy(t, d, r).start()

    for j in range(IN_CHUNKS):
        for d in range(2):
            ring(d, 0, j).start()
    for j in range(IN_CHUNKS):
        ref = own_slot.at[:, piece(j)]
        remote(ref, ref, pair_send_sem.at[0, half], pair_sem.at[0, half], pair).start()
    for load in loads[2:]:
        load.start()
    wo_copy = remote(w_out.at[:, half_cols(other)], wo.at[c], wo_send_sem, wo_sem, pair)
    wo_copy.start()

    def gather_step(s):
        known = isinstance(s, int)
        before = half if known and s == 0 else s - 1
        for j in range(IN_CHUNKS):
            for d in range(2):
                if not known or travels(d, s, j):
                    ring(d, s, j).wait_recv()
                    if not known or (s < half - 1 and travels(d, s + 1, j)):
                        ring(d, s + 1, j).start()
                    to_pair(d, s, j).start()
            if known and s == 0 and j == 0:
                loads[1].wait()
            dot_piece(before, j)
        send_parts(before)
        if not known or s > 0:
            send_queries(half if known and s == 1 else s - 2)

    gather_step(0)
    gather_step(1)

    @pl.loop(2, half - 2)
    def _(s):
        gather_step(s)

    for s in range(max(half - 2, 2), half):
        gather_step(s)
    for j in range(IN_CHUNKS):
        dot_piece(half - 1, j)
    heads = CORES * feats // hd

    def scores_of(i, lo, hi):
        rows = jnp.concatenate([q_wide[lo:hi, core, i, :] for core in range(CORES)], axis=1)
        query = jnp.concatenate([rows[:, h * hd : (h + 1) * hd] for h in range(heads)], axis=0).astype(BF16)
        return lax.dot_general(query, k_buf[i], (((1,), (1,)), ((), ())), preferred_element_type=F32)

    def probs_of(i, scores):
        scores = scores * F32(hd**-0.5)
        live = lax.broadcasted_iota(jnp.int32, scores.shape, 1) < lengths[i]
        scores = jnp.where(live, scores, F32(-1e30))
        expo = jnp.where(live, jnp.exp(scores - jnp.max(scores, axis=1, keepdims=True)), F32(0.0))
        return (expo / jnp.sum(expo, axis=1, keepdims=True)).astype(BF16)

    def att_copy(v, r):
        core = lax.rem(c + r, CORES)
        slot = v if v in (0, nz - 1) else v + 1 if v % 2 else v - 1
        return remote(
            att_send.at[v, core],
            att_in.at[x, slot, c],
            att_send_sem.at[r],
            att_sem.at[slot, c],
            at_z(z + source_offset(v, half), core),
        )

    def attend(lo, hi):
        for v in range(lo, hi):
            for r in range(CORES):
                core = lax.rem(c + r, CORES)
                if v < nz - 1 or r > 0:
                    ref = q_in.at[v, core]
                    remote(ref, ref, q_send_sem.at[r], q_sem.at[v, core], pair).wait_recv()
        q_wide[lo:hi] = q_in[lo:hi].astype(F32)
        scores = [scores_of(i, lo, hi) for i in range(seqs)]
        probs = [probs_of(i, scores[i]) for i in range(seqs)]
        mixed = [jnp.dot(probs[i], v_buf[i], preferred_element_type=F32) for i in range(seqs)]
        for i in range(seqs):
            wide = jnp.concatenate(
                [mixed[i][h * (hi - lo) : (h + 1) * (hi - lo), :] for h in range(heads)], axis=1
            )
            for core in range(CORES):
                att_wide[lo:hi, core, i, :] = wide[:, core * feats : (core + 1) * feats]
        att_send[lo:hi] = att_wide[lo:hi].astype(BF16)
        for v in range(lo, hi):
            for r in range(CORES):
                if v == nz - 1 and r == 0:
                    att_in[x, v, c] = att_send[v, c]
                else:
                    att_copy(v, r).start()

    send_parts(half - 1)
    send_queries(half - 2)
    for load in loads[3:]:
        load.wait()
    attend(nz // 2, nz)
    send_queries(half - 1)
    attend(nz // 4, nz // 2)
    attend(0, nz // 4)

    own_batch = nz // PER_BATCH + 1

    def batch(b):
        known = isinstance(b, int)
        if known and b in (0, own_batch):
            return (0 if b == 0 else nz - 1), 1
        return (1, 2) if known and b == 1 else (PER_BATCH * b - 5, PER_BATCH)

    def rows_copy(b, k):
        ref = att_in.at[x, pl.ds(*batch(b))]
        return remote(ref, ref, rows_send_sem.at[b, k - 1], rows_sem.at[b, k - 1], at_x(k))

    def swap_copy(b):
        ref = att.at[c, pl.ds(*batch(b))]
        return remote(ref, ref, swap_send_sem.at[b], swap_sem.at[b], pair)

    def pass_on(b):
        for k in range(1, nx):
            rows_copy(b, k).wait_recv()
        start, count = batch(b)
        for n in range(count):
            for core in range(CORES):
                v = start + n
                att[c, v, core] = jnp.concatenate(
                    [att_in[g, v, core].astype(F32) for g in range(nx)], axis=0
                ).astype(BF16)
        swap_copy(b).start()

    for b in range(own_batch + 1):
        start, count = batch(b)
        for v in range(start, start + count):
            for r in range(CORES):
                core = lax.rem(c + r, CORES)
                if v < nz - 1 or r > 0:
                    ref = att_in.at[x, v, core]
                    remote(ref, ref, att_send_sem.at[r], att_sem.at[v, core], pair).wait_recv()
        for k in range(1, nx):
            rows_copy(b, k).start()
    pass_on(0)
    loads[2].wait()
    wo_copy.wait_recv()

    def out_piece(j):
        return pl.ds(j * out_cols, out_cols)

    def projected(v, count, j):
        lhs = jnp.concatenate(
            [att[f, pl.ds(v, count)].reshape(count * CORES * block, feats) for f in range(CORES)], axis=1
        )
        rhs = wo[:, :, j * out_cols : (j + 1) * out_cols].reshape(CORES * feats, out_cols)
        return jnp.dot(lhs, rhs, preferred_element_type=F32)

    def sums_copy(d, s, j):
        return remote(
            sums.at[d, s, :, out_piece(j)],
            sums_in.at[d, s, :, out_piece(j)],
            sums_send_sem.at[d, s],
            sums_sem.at[d, s, j],
            side[d],
        )

    def starts(d, j):
        return (j < (OUT_CHUNKS + 1) // 2) == (d == 0)

    tall = CORES * block

    def out_step(s):
        known = isinstance(s, int)
        for j in range(OUT_CHUNKS):
            span = slice(j * out_cols, (j + 1) * out_cols)
            if known and s == 0:
                d = 0 if starts(0, j) else 1
                sums[d, 0, :, span] = projected(0, 1, j).astype(BF16)
                sums_copy(d, 0, j).start()
                continue
            both = projected(2 * s - 1, 2, j)
            for d in range(2):
                term = both[d * tall : (d + 1) * tall]
                if not known or s > 1 or starts(d, j):
                    sums_copy(d, s - 1, j).wait_recv()
                    term = term + sums_in[d, s - 1, :, span].astype(F32)
                sums[d, s, :, span] = term.astype(BF16)
                sums_copy(d, s, j).start()

    pass_on(1)
    swap_copy(0).wait_recv()
    out_step(0)
    pass_on(2)
    swap_copy(1).wait_recv()
    out_step(1)

    @pl.loop(2, own_batch - 1)
    def _(b):
        pass_on(b + 1)
        swap_copy(b).wait_recv()
        out_step(2 * b - 2)
        out_step(2 * b - 1)

    pass_on(own_batch)
    swap_copy(own_batch - 1).wait_recv()

    @pl.loop(half - 2, half)
    def _(s):
        out_step(s)

    swap_copy(own_batch).wait_recv()

    def last_copy(j):
        own = pl.ds(pl.multiple_of(c * own_cols + j * out_cols, 128), out_cols)
        return remote(
            last.at[other, :, out_piece(j)], out.at[:, own], last_send_sem.at[j], last_sem.at[j], pair
        )

    for j in range(OUT_CHUNKS):
        span = slice(j * out_cols, (j + 1) * out_cols)
        term = projected(nz - 1, 1, j)
        for d in range(2):
            sums_copy(d, half - 1, j).wait_recv()
            term = term + sums_in[d, half - 1, :, span].astype(F32)
        for core in range(CORES):
            last[core, :, span] = term[core * block : (core + 1) * block].astype(BF16)
        last_copy(j).start()
    out[:, half_cols(c)] = last[c]
    for j in range(OUT_CHUNKS):
        last_copy(j).wait_recv()

    def left(ref, sem, recv_sem, device):
        remote(ref, ref, sem, recv_sem, device).wait_send()

    @pl.loop(0, half - 1)
    def _(t):
        for d in range(2):
            left(gathered.at[0, c], pair_send_sem.at[d, t], pair_sem.at[d, t], pair)
            left(gathered.at[0, c], ring_send_sem.at[d, t], ring_sem.at[d, t, 0], side[d])
        for k in range(1, nx):
            part_copy(t, k).wait_send()

    for t in (half - 1, half):
        left(gathered.at[0, c], pair_send_sem.at[0, t], pair_sem.at[0, t], pair)
        for k in range(1, nx):
            part_copy(t, k).wait_send()

    @pl.loop(1, half)
    def _(s):
        for d in range(2):
            left(sums.at[d, s], sums_send_sem.at[d, s], sums_sem.at[d, s, 0], side[d])

    for d in range(2):
        left(
            gathered.at[0, c, :, pl.ds(0, width // 2)], ring_send_sem.at[d, half - 1], ring_sem.at[d, half - 1, 0], side[d]
        )
        first = out_cols * sum(starts(d, j) for j in range(OUT_CHUNKS))
        left(sums.at[d, 0, :, pl.ds(0, first)], sums_send_sem.at[d, 0], sums_sem.at[d, 0, 0], side[d])
    for r in range(CORES):
        ref = q_in.at[pl.ds(0, nz - 1 + r), 0]
        left(ref, q_send_sem.at[r], q_sem.at[0, 0], pair)
        left(ref, att_send_sem.at[r], att_sem.at[0, 0], pair)
    for b in range(own_batch + 1):
        swap_copy(b).wait_send()
        for k in range(1, nx):
            rows_copy(b, k).wait_send()
    wo_copy.wait_send()
    for j in range(OUT_CHUNKS):
        last_copy(j).wait_send()


def solution(mesh):
    nz = mesh.shape["gx"] // CORES
    nx = mesh.shape["gy"]
    half = nz // 2

    def body(hidden_in, w_query, w_out, cache_keys, cache_values, lengths):
        block, width = hidden_in.shape
        feats = w_query.shape[1]
        seqs, slots, hd = cache_keys.shape
        own_cols = width // CORES
        dma = pltpu.SemaphoreType.DMA
        hbm = pl.BlockSpec(memory_space=pltpu.HBM)
        return pl.pallas_call(
            functools.partial(kernel, nz, nx),
            out_shape=jax.ShapeDtypeStruct((block, width), BF16),
            in_specs=[pl.BlockSpec(memory_space=pltpu.SMEM)] + [hbm] * 5,
            out_specs=pl.BlockSpec(memory_space=pltpu.VMEM),
            scratch_shapes=[
                pltpu.VMEM((half + 1, 2 * CORES, block, width), BF16),
                pltpu.VMEM(w_query.shape, BF16),
                pltpu.VMEM((CORES, feats, own_cols), BF16),
                pltpu.VMEM(cache_keys.shape, BF16),
                pltpu.VMEM(cache_values.shape, BF16),
                pltpu.VMEM((2 * CORES * block, feats), F32),
                pltpu.VMEM((half + 1, nx, 2 * CORES * seqs, feats), F32),
                pltpu.VMEM((half + 1, nx - 1, 2 * CORES * seqs, feats), F32),
                pltpu.VMEM((half + 1, 2 * CORES, seqs, feats), BF16),
                pltpu.VMEM((nz, CORES, seqs, feats), BF16),
                pltpu.VMEM((nz, CORES, seqs, feats), F32),
                pltpu.VMEM((nz, CORES, seqs, feats), F32),
                pltpu.VMEM((nz, CORES, seqs, feats), BF16),
                pltpu.VMEM((nx, nz, CORES, seqs, feats), BF16),
                pltpu.VMEM((CORES, nz, CORES, block, feats), BF16),
                pltpu.VMEM((2, half, CORES * block, own_cols), BF16),
                pltpu.VMEM((2, half, CORES * block, own_cols), BF16),
                pltpu.VMEM((CORES, block, own_cols), BF16),
                dma((5,)),
                dma((2, half)),
                dma((2, half, IN_CHUNKS)),
                dma((2, half + 1)),
                dma((2, half + 1)),
                dma((half + 1, nx - 1)),
                dma((half + 1, nx - 1)),
                dma((CORES,)),
                dma((nz, CORES)),
                dma((CORES,)),
                dma((nz, CORES)),
                dma((nz // PER_BATCH + 2, nx - 1)),
                dma((nz // PER_BATCH + 2, nx - 1)),
                dma((nz // PER_BATCH + 2,)),
                dma((nz // PER_BATCH + 2,)),
                dma(()),
                dma(()),
                dma((2, half)),
                dma((2, half, OUT_CHUNKS)),
                dma((OUT_CHUNKS,)),
                dma((OUT_CHUNKS,)),
            ],
            compiler_params=pltpu.CompilerParams(
                collective_id=0, has_side_effects=True, vmem_limit_bytes=52 * 2**20
            ),
            name="decode_step",
        )(lengths, hidden_in, w_query, w_out, cache_keys, cache_values)

    return jax.shard_map(
        body,
        mesh=mesh,
        in_specs=(
            P(("groups", "gx"), "gy"),
            P("gy", "gx"),
            P("gx", "gy"),
            P(("groups", "gx", "gy"), None, None),
            P(("groups", "gx", "gy"), None, None),
            P(("groups", "gx", "gy")),
        ),
        out_specs=P(("groups", "gx"), "gy"),
        check_vma=False,
    )
```

```python
import functools

import jax
import jax.numpy as jnp
from jax import lax
from jax.experimental import pallas as pl
from jax.experimental.pallas import tpu as pltpu
from jax.sharding import PartitionSpec as P

MESH = pl.DeviceIdType.MESH
CORES = 2
IN_CHUNKS = 6
OUT_CHUNKS = 6
PER_BATCH = 4
F32 = jnp.float32
BF16 = jnp.bfloat16


def source_offset(v, half):
    return half - (v + 1) // 2 if v % 2 else half + v // 2


def kernel(
    nz,
    nx,
    lengths,
    hidden,
    w_query,
    w_out,
    keys,
    values,
    out,
    gathered,
    wq,
    wo,
    k_buf,
    v_buf,
    acc,
    part,
    part_in,
    q_send,
    q_in,
    q_wide,
    att_wide,
    att_send,
    att_in,
    att,
    sums,
    sums_in,
    last,
    local_sem,
    ring_send_sem,
    ring_sem,
    pair_send_sem,
    pair_sem,
    part_send_sem,
    part_sem,
    q_send_sem,
    q_sem,
    att_send_sem,
    att_sem,
    rows_send_sem,
    rows_sem,
    swap_send_sem,
    swap_sem,
    wo_send_sem,
    wo_sem,
    sums_send_sem,
    sums_sem,
    last_send_sem,
    last_sem,
):
    half = nz // 2
    gx = lax.axis_index("gx")
    x = lax.axis_index("gy")
    z = gx // CORES
    c = gx % CORES
    other = 1 - c
    seqs, slots, hd = k_buf.shape
    width = hidden.shape[1]
    cols = width // IN_CHUNKS
    own_cols = width // CORES
    out_cols = own_cols // OUT_CHUNKS
    feats = w_query.shape[1]
    block = nx * seqs

    def at_z(chip, core):
        return {"gx": lax.rem(chip + 2 * nz, nz) * CORES + core}

    def at_x(offset):
        return {"gy": lax.rem(x + offset, nx)}

    side = (at_z(z + 1, c), at_z(z - 1, c))
    pair = {"gx": z * CORES + other}

    def remote(src, dst, send_sem, recv_sem, device):
        return pltpu.make_async_remote_copy(
            src_ref=src, dst_ref=dst, send_sem=send_sem, recv_sem=recv_sem, device_id=device, device_id_type=MESH
        )

    def half_cols(core):
        return pl.ds(pl.multiple_of(core * own_cols, 128), own_cols)

    own_slot = gathered.at[half, c]
    loads = [
        pltpu.make_async_copy(hidden, own_slot, local_sem.at[0]),
        pltpu.make_async_copy(w_query, wq, local_sem.at[1]),
        pltpu.make_async_copy(w_out.at[:, half_cols(c)], wo.at[c], local_sem.at[2]),
        pltpu.make_async_copy(keys, k_buf, local_sem.at[3]),
        pltpu.make_async_copy(values, v_buf, local_sem.at[4]),
    ]
    loads[0].start()
    loads[1].start()

    barrier = pltpu.get_barrier_semaphore()
    greeted = [*side, pair] + [at_x(k) for k in range(1, nx)]
    for device in greeted:
        pl.semaphore_signal(barrier, inc=1, device_id=device, device_id_type=MESH)
    pl.semaphore_wait(barrier, len(greeted))
    loads[0].wait()

    def piece(j):
        return pl.ds(j * cols, cols)

    def home(s, d):
        return 0 if isinstance(s, int) and s == half - 1 else d

    def ring(d, s, j):
        src = own_slot if isinstance(s, int) and s == 0 else gathered.at[s - 1, CORES * d + c]
        dst = gathered.at[s, CORES * home(s, d) + c]
        return remote(src.at[:, piece(j)], dst.at[:, piece(j)], ring_send_sem.at[d, s], ring_sem.at[d, s, j], side[d])

    def to_pair(d, s, j):
        ref = gathered.at[s, CORES * home(s, d) + c, :, piece(j)]
        return remote(ref, ref, pair_send_sem.at[home(s, d), s], pair_sem.at[home(s, d), s], pair)

    def travels(d, s, j):
        return s < half - 1 or (j < IN_CHUNKS // 2) == (d == 0)

    def blocks(t):
        return CORES if isinstance(t, int) and t >= half - 1 else 2 * CORES

    def dot_piece(t, j):
        if j == 0:
            for d in range(blocks(t) // CORES):
                ref = gathered.at[t, CORES * d + other]
                remote(ref, ref, pair_send_sem.at[d, t], pair_sem.at[d, t], pair).wait_recv()
        tall = blocks(t) * block
        lhs = gathered[t, : blocks(t), :, j * cols : (j + 1) * cols].reshape(tall, cols)
        term = jnp.dot(lhs, wq[j * cols : (j + 1) * cols, :], preferred_element_type=F32)
        if j == 0:
            acc[:tall] = term
        else:
            acc[:tall] += term

    def part_copy(t, k):
        rows = pl.ds(0, blocks(t) * seqs)
        return remote(
            part.at[t, lax.rem(x + k, nx), rows],
            part_in.at[t, k - 1, rows],
            part_send_sem.at[t, k - 1],
            part_sem.at[t, k - 1],
            at_x(k),
        )

    def send_parts(t):
        for g in range(nx):
            part[t, g, : blocks(t) * seqs] = jnp.concatenate(
                [acc[b * block + g * seqs : b * block + (g + 1) * seqs, :] for b in range(blocks(t))], axis=0
            )
        for k in range(1, nx):
            part_copy(t, k).start()

    def q_copy(t, d, r):
        core = lax.rem(c + r, CORES)
        if isinstance(t, int) and t >= half - 1:
            chip = z if t == half else z + half
        else:
            chip = z - 1 - t if d == 0 else z + 1 + t
        slot = 2 * (half - 1 - t) - 1 + d
        if isinstance(t, int) and t >= half - 1:
            slot = nz - 1 if t == half else 0
        return remote(
            q_send.at[t, CORES * d + core], q_in.at[slot, c], q_send_sem.at[r], q_sem.at[slot, c], at_z(chip, core)
        )

    def send_queries(t):
        rows = blocks(t) * seqs
        total = part[t, x, :rows]
        for k in range(1, nx):
            part_copy(t, k).wait_recv()
            total = total + part_in[t, k - 1, :rows]
        for b in range(blocks(t)):
            q_send[t, b] = total[b * seqs : (b + 1) * seqs, :].astype(BF16)
        for d in range(blocks(t) // CORES):
            for r in range(CORES):
                if isinstance(t, int) and t == half and r == 0:
                    q_in[nz - 1, c] = q_send[half, c]
                else:
                    q_copy(t, d, r).start()

    for j in range(IN_CHUNKS):
        for d in range(2):
            ring(d, 0, j).start()
    for j in range(IN_CHUNKS):
        ref = own_slot.at[:, piece(j)]
        remote(ref, ref, pair_send_sem.at[0, half], pair_sem.at[0, half], pair).start()
    for load in loads[2:]:
        load.start()
    wo_copy = remote(w_out.at[:, half_cols(other)], wo.at[c], wo_send_sem, wo_sem, pair)
    wo_copy.start()

    def gather_step(s):
        known = isinstance(s, int)
        before = half if known and s == 0 else s - 1
        for j in range(IN_CHUNKS):
            for d in range(2):
                if not known or travels(d, s, j):
                    ring(d, s, j).wait_recv()
                    if not known or (s < half - 1 and travels(d, s + 1, j)):
                        ring(d, s + 1, j).start()
                    to_pair(d, s, j).start()
            if known and s == 0 and j == 0:
                loads[1].wait()
            dot_piece(before, j)
        send_parts(before)
        if not known or s > 0:
            send_queries(half if known and s == 1 else s - 2)

    gather_step(0)
    gather_step(1)

    @pl.loop(2, half - 2)
    def _(s):
        gather_step(s)

    for s in range(max(half - 2, 2), half):
        gather_step(s)
    for j in range(IN_CHUNKS):
        dot_piece(half - 1, j)
    heads = CORES * feats // hd

    def scores_of(i, lo, hi):
        rows = jnp.concatenate([q_wide[lo:hi, core, i, :] for core in range(CORES)], axis=1)
        query = jnp.concatenate([rows[:, h * hd : (h + 1) * hd] for h in range(heads)], axis=0).astype(BF16)
        return lax.dot_general(query, k_buf[i], (((1,), (1,)), ((), ())), preferred_element_type=F32)

    def probs_of(i, scores):
        scores = scores * F32(hd**-0.5)
        live = lax.broadcasted_iota(jnp.int32, scores.shape, 1) < lengths[i]
        scores = jnp.where(live, scores, F32(-1e30))
        expo = jnp.where(live, jnp.exp(scores - jnp.max(scores, axis=1, keepdims=True)), F32(0.0))
        return (expo / jnp.sum(expo, axis=1, keepdims=True)).astype(BF16)

    def att_copy(v, r):
        core = lax.rem(c + r, CORES)
        slot = v if v in (0, nz - 1) else v + 1 if v % 2 else v - 1
        return remote(
            att_send.at[v, core],
            att_in.at[x, slot, c],
            att_send_sem.at[r],
            att_sem.at[slot, c],
            at_z(z + source_offset(v, half), core),
        )

    def attend(lo, hi):
        for v in range(lo, hi):
            for r in range(CORES):
                core = lax.rem(c + r, CORES)
                if v < nz - 1 or r > 0:
                    ref = q_in.at[v, core]
                    remote(ref, ref, q_send_sem.at[r], q_sem.at[v, core], pair).wait_recv()
        q_wide[lo:hi] = q_in[lo:hi].astype(F32)
        scores = [scores_of(i, lo, hi) for i in range(seqs)]
        probs = [probs_of(i, scores[i]) for i in range(seqs)]
        mixed = [jnp.dot(probs[i], v_buf[i], preferred_element_type=F32) for i in range(seqs)]
        for i in range(seqs):
            wide = jnp.concatenate(
                [mixed[i][h * (hi - lo) : (h + 1) * (hi - lo), :] for h in range(heads)], axis=1
            )
            for core in range(CORES):
                att_wide[lo:hi, core, i, :] = wide[:, core * feats : (core + 1) * feats]
        att_send[lo:hi] = att_wide[lo:hi].astype(BF16)
        for v in range(lo, hi):
            for r in range(CORES):
                if v == nz - 1 and r == 0:
                    att_in[x, v, c] = att_send[v, c]
                else:
                    att_copy(v, r).start()

    send_parts(half - 1)
    send_queries(half - 2)
    for load in loads[3:]:
        load.wait()
    send_queries(half - 1)
    attend(nz // 4, nz)
    attend(0, nz // 4)

    own_batch = nz // PER_BATCH + 1

    def batch(b):
        known = isinstance(b, int)
        if known and b in (0, own_batch):
            return (0 if b == 0 else nz - 1), 1
        return (1, 2) if known and b == 1 else (PER_BATCH * b - 5, PER_BATCH)

    def rows_copy(b, k):
        ref = att_in.at[x, pl.ds(*batch(b))]
        return remote(ref, ref, rows_send_sem.at[b, k - 1], rows_sem.at[b, k - 1], at_x(k))

    def swap_copy(b):
        ref = att.at[c, pl.ds(*batch(b))]
        return remote(ref, ref, swap_send_sem.at[b], swap_sem.at[b], pair)

    def pass_on(b):
        for k in range(1, nx):
            rows_copy(b, k).wait_recv()
        start, count = batch(b)
        for n in range(count):
            for core in range(CORES):
                v = start + n
                att[c, v, core] = jnp.concatenate(
                    [att_in[g, v, core].astype(F32) for g in range(nx)], axis=0
                ).astype(BF16)
        swap_copy(b).start()

    for b in range(own_batch + 1):
        start, count = batch(b)
        for v in range(start, start + count):
            for r in range(CORES):
                core = lax.rem(c + r, CORES)
                if v < nz - 1 or r > 0:
                    ref = att_in.at[x, v, core]
                    remote(ref, ref, att_send_sem.at[r], att_sem.at[v, core], pair).wait_recv()
        for k in range(1, nx):
            rows_copy(b, k).start()
    pass_on(0)
    loads[2].wait()
    wo_copy.wait_recv()

    def out_piece(j):
        return pl.ds(j * out_cols, out_cols)

    def projected(v, count, j):
        lhs = jnp.concatenate(
            [att[f, pl.ds(v, count)].reshape(count * CORES * block, feats) for f in range(CORES)], axis=1
        )
        rhs = wo[:, :, j * out_cols : (j + 1) * out_cols].reshape(CORES * feats, out_cols)
        return jnp.dot(lhs, rhs, preferred_element_type=F32)

    def sums_copy(d, s, j):
        return remote(
            sums.at[d, s, :, out_piece(j)],
            sums_in.at[d, s, :, out_piece(j)],
            sums_send_sem.at[d, s],
            sums_sem.at[d, s, j],
            side[d],
        )

    def starts(d, j):
        return (j < (OUT_CHUNKS + 1) // 2) == (d == 0)

    tall = CORES * block

    def out_step(s):
        known = isinstance(s, int)
        for j in range(OUT_CHUNKS):
            span = slice(j * out_cols, (j + 1) * out_cols)
            if known and s == 0:
                d = 0 if starts(0, j) else 1
                sums[d, 0, :, span] = projected(0, 1, j).astype(BF16)
                sums_copy(d, 0, j).start()
                continue
            both = projected(2 * s - 1, 2, j)
            for d in range(2):
                term = both[d * tall : (d + 1) * tall]
                if not known or s > 1 or starts(d, j):
                    sums_copy(d, s - 1, j).wait_recv()
                    term = term + sums_in[d, s - 1, :, span].astype(F32)
                sums[d, s, :, span] = term.astype(BF16)
                sums_copy(d, s, j).start()

    pass_on(1)
    swap_copy(0).wait_recv()
    out_step(0)
    pass_on(2)
    swap_copy(1).wait_recv()
    out_step(1)

    @pl.loop(2, own_batch - 1)
    def _(b):
        pass_on(b + 1)
        swap_copy(b).wait_recv()
        out_step(2 * b - 2)
        out_step(2 * b - 1)

    pass_on(own_batch)
    swap_copy(own_batch - 1).wait_recv()

    @pl.loop(half - 2, half)
    def _(s):
        out_step(s)

    swap_copy(own_batch).wait_recv()

    def last_copy(j):
        own = pl.ds(pl.multiple_of(c * own_cols + j * out_cols, 128), out_cols)
        return remote(
            last.at[other, :, out_piece(j)], out.at[:, own], last_send_sem.at[j], last_sem.at[j], pair
        )

    for j in range(OUT_CHUNKS):
        span = slice(j * out_cols, (j + 1) * out_cols)
        term = projected(nz - 1, 1, j)
        for d in range(2):
            sums_copy(d, half - 1, j).wait_recv()
            term = term + sums_in[d, half - 1, :, span].astype(F32)
        for core in range(CORES):
            last[core, :, span] = term[core * block : (core + 1) * block].astype(BF16)
        last_copy(j).start()
    out[:, half_cols(c)] = last[c]
    for j in range(OUT_CHUNKS):
        last_copy(j).wait_recv()

    def left(ref, sem, recv_sem, device):
        remote(ref, ref, sem, recv_sem, device).wait_send()

    @pl.loop(0, half - 1)
    def _(t):
        for d in range(2):
            left(gathered.at[0, c], pair_send_sem.at[d, t], pair_sem.at[d, t], pair)
            left(gathered.at[0, c], ring_send_sem.at[d, t], ring_sem.at[d, t, 0], side[d])
        for k in range(1, nx):
            part_copy(t, k).wait_send()

    for t in (half - 1, half):
        left(gathered.at[0, c], pair_send_sem.at[0, t], pair_sem.at[0, t], pair)
        for k in range(1, nx):
            part_copy(t, k).wait_send()

    @pl.loop(1, half)
    def _(s):
        for d in range(2):
            left(sums.at[d, s], sums_send_sem.at[d, s], sums_sem.at[d, s, 0], side[d])

    for d in range(2):
        left(
            gathered.at[0, c, :, pl.ds(0, width // 2)], ring_send_sem.at[d, half - 1], ring_sem.at[d, half - 1, 0], side[d]
        )
        first = out_cols * sum(starts(d, j) for j in range(OUT_CHUNKS))
        left(sums.at[d, 0, :, pl.ds(0, first)], sums_send_sem.at[d, 0], sums_sem.at[d, 0, 0], side[d])
    for r in range(CORES):
        ref = q_in.at[pl.ds(0, nz - 1 + r), 0]
        left(ref, q_send_sem.at[r], q_sem.at[0, 0], pair)
        left(ref, att_send_sem.at[r], att_sem.at[0, 0], pair)
    for b in range(own_batch + 1):
        swap_copy(b).wait_send()
        for k in range(1, nx):
            rows_copy(b, k).wait_send()
    wo_copy.wait_send()
    for j in range(OUT_CHUNKS):
        last_copy(j).wait_send()


def solution(mesh):
    nz = mesh.shape["gx"] // CORES
    nx = mesh.shape["gy"]
    half = nz // 2

    def body(hidden_in, w_query, w_out, cache_keys, cache_values, lengths):
        block, width = hidden_in.shape
        feats = w_query.shape[1]
        seqs, slots, hd = cache_keys.shape
        own_cols = width // CORES
        dma = pltpu.SemaphoreType.DMA
        hbm = pl.BlockSpec(memory_space=pltpu.HBM)
        return pl.pallas_call(
            functools.partial(kernel, nz, nx),
            out_shape=jax.ShapeDtypeStruct((block, width), BF16),
            in_specs=[pl.BlockSpec(memory_space=pltpu.SMEM)] + [hbm] * 5,
            out_specs=pl.BlockSpec(memory_space=pltpu.VMEM),
            scratch_shapes=[
                pltpu.VMEM((half + 1, 2 * CORES, block, width), BF16),
                pltpu.VMEM(w_query.shape, BF16),
                pltpu.VMEM((CORES, feats, own_cols), BF16),
                pltpu.VMEM(cache_keys.shape, BF16),
                pltpu.VMEM(cache_values.shape, BF16),
                pltpu.VMEM((2 * CORES * block, feats), F32),
                pltpu.VMEM((half + 1, nx, 2 * CORES * seqs, feats), F32),
                pltpu.VMEM((half + 1, nx - 1, 2 * CORES * seqs, feats), F32),
                pltpu.VMEM((half + 1, 2 * CORES, seqs, feats), BF16),
                pltpu.VMEM((nz, CORES, seqs, feats), BF16),
                pltpu.VMEM((nz, CORES, seqs, feats), F32),
                pltpu.VMEM((nz, CORES, seqs, feats), F32),
                pltpu.VMEM((nz, CORES, seqs, feats), BF16),
                pltpu.VMEM((nx, nz, CORES, seqs, feats), BF16),
                pltpu.VMEM((CORES, nz, CORES, block, feats), BF16),
                pltpu.VMEM((2, half, CORES * block, own_cols), BF16),
                pltpu.VMEM((2, half, CORES * block, own_cols), BF16),
                pltpu.VMEM((CORES, block, own_cols), BF16),
                dma((5,)),
                dma((2, half)),
                dma((2, half, IN_CHUNKS)),
                dma((2, half + 1)),
                dma((2, half + 1)),
                dma((half + 1, nx - 1)),
                dma((half + 1, nx - 1)),
                dma((CORES,)),
                dma((nz, CORES)),
                dma((CORES,)),
                dma((nz, CORES)),
                dma((nz // PER_BATCH + 2, nx - 1)),
                dma((nz // PER_BATCH + 2, nx - 1)),
                dma((nz // PER_BATCH + 2,)),
                dma((nz // PER_BATCH + 2,)),
                dma(()),
                dma(()),
                dma((2, half)),
                dma((2, half, OUT_CHUNKS)),
                dma((OUT_CHUNKS,)),
                dma((OUT_CHUNKS,)),
            ],
            compiler_params=pltpu.CompilerParams(
                collective_id=0, has_side_effects=True, vmem_limit_bytes=215 * 2**18
            ),
            name="decode_step",
        )(lengths, hidden_in, w_query, w_out, cache_keys, cache_values)

    return jax.shard_map(
        body,
        mesh=mesh,
        in_specs=(
            P(("groups", "gx"), "gy"),
            P("gy", "gx"),
            P("gx", "gy"),
            P(("groups", "gx", "gy"), None, None),
            P(("groups", "gx", "gy"), None, None),
            P(("groups", "gx", "gy")),
        ),
        out_specs=P(("groups", "gx"), "gy"),
        check_vma=False,
    )
```

```python
import functools

import jax
import jax.numpy as jnp
from jax import lax
from jax.experimental import pallas as pl
from jax.experimental.pallas import tpu as pltpu
from jax.sharding import PartitionSpec as P

MESH = pl.DeviceIdType.MESH
CORES = 2
IN_CHUNKS = 6
OUT_CHUNKS = 6
PER_BATCH = 4
F32 = jnp.float32
BF16 = jnp.bfloat16


def source_offset(v, half):
    return half - (v + 1) // 2 if v % 2 else half + v // 2


def kernel(
    nz,
    nx,
    lengths,
    hidden,
    w_query,
    w_out,
    keys,
    values,
    out,
    gathered,
    wq,
    wo,
    k_buf,
    v_buf,
    acc,
    part,
    part_in,
    q_send,
    q_in,
    q_wide,
    att_wide,
    att_send,
    att_in,
    att,
    sums,
    sums_in,
    last,
    local_sem,
    ring_send_sem,
    ring_sem,
    pair_send_sem,
    pair_sem,
    part_send_sem,
    part_sem,
    q_send_sem,
    q_sem,
    att_send_sem,
    att_sem,
    far_send_sem,
    far_sem,
    rows_send_sem,
    rows_sem,
    swap_send_sem,
    swap_sem,
    wo_send_sem,
    wo_sem,
    sums_send_sem,
    sums_sem,
    last_send_sem,
    last_sem,
):
    half = nz // 2
    gx = lax.axis_index("gx")
    x = lax.axis_index("gy")
    z = gx // CORES
    c = gx % CORES
    other = 1 - c
    seqs, slots, hd = k_buf.shape
    width = hidden.shape[1]
    cols = width // IN_CHUNKS
    own_cols = width // CORES
    out_cols = own_cols // OUT_CHUNKS
    feats = w_query.shape[1]
    block = nx * seqs

    def at_z(chip, core):
        return {"gx": lax.rem(chip + 2 * nz, nz) * CORES + core}

    def at_x(offset):
        return {"gy": lax.rem(x + offset, nx)}

    side = (at_z(z + 1, c), at_z(z - 1, c))
    pair = {"gx": z * CORES + other}

    def remote(src, dst, send_sem, recv_sem, device):
        return pltpu.make_async_remote_copy(
            src_ref=src, dst_ref=dst, send_sem=send_sem, recv_sem=recv_sem, device_id=device, device_id_type=MESH
        )

    def half_cols(core):
        return pl.ds(pl.multiple_of(core * own_cols, 128), own_cols)

    own_slot = gathered.at[half, c]
    loads = [
        pltpu.make_async_copy(hidden, own_slot, local_sem.at[0]),
        pltpu.make_async_copy(w_query, wq, local_sem.at[1]),
        pltpu.make_async_copy(w_out.at[:, half_cols(c)], wo.at[c], local_sem.at[2]),
        pltpu.make_async_copy(keys, k_buf, local_sem.at[3]),
        pltpu.make_async_copy(values, v_buf, local_sem.at[4]),
    ]
    loads[0].start()
    loads[1].start()

    barrier = pltpu.get_barrier_semaphore()
    greeted = [*side, pair] + [at_x(k) for k in range(1, nx)]
    for device in greeted:
        pl.semaphore_signal(barrier, inc=1, device_id=device, device_id_type=MESH)
    pl.semaphore_wait(barrier, len(greeted))
    loads[0].wait()

    def piece(j):
        return pl.ds(j * cols, cols)

    def home(s, d):
        return 0 if isinstance(s, int) and s == half - 1 else d

    def ring(d, s, j):
        src = own_slot if isinstance(s, int) and s == 0 else gathered.at[s - 1, CORES * d + c]
        dst = gathered.at[s, CORES * home(s, d) + c]
        return remote(src.at[:, piece(j)], dst.at[:, piece(j)], ring_send_sem.at[d, s], ring_sem.at[d, s, j], side[d])

    def to_pair(d, s, j):
        ref = gathered.at[s, CORES * home(s, d) + c, :, piece(j)]
        return remote(ref, ref, pair_send_sem.at[home(s, d), s], pair_sem.at[home(s, d), s], pair)

    def travels(d, s, j):
        return s < half - 1 or (j < IN_CHUNKS // 2) == (d == 0)

    def blocks(t):
        return CORES if isinstance(t, int) and t >= half - 1 else 2 * CORES

    def dot_piece(t, j):
        if j == 0:
            for d in range(blocks(t) // CORES):
                ref = gathered.at[t, CORES * d + other]
                remote(ref, ref, pair_send_sem.at[d, t], pair_sem.at[d, t], pair).wait_recv()
        tall = blocks(t) * block
        lhs = gathered[t, : blocks(t), :, j * cols : (j + 1) * cols].reshape(tall, cols)
        term = jnp.dot(lhs, wq[j * cols : (j + 1) * cols, :], preferred_element_type=F32)
        if j == 0:
            acc[:tall] = term
        else:
            acc[:tall] += term

    def part_copy(t, k):
        rows = pl.ds(0, blocks(t) * seqs)
        return remote(
            part.at[t, lax.rem(x + k, nx), rows],
            part_in.at[t, k - 1, rows],
            part_send_sem.at[t, k - 1],
            part_sem.at[t, k - 1],
            at_x(k),
        )

    def send_parts(t):
        for g in range(nx):
            part[t, g, : blocks(t) * seqs] = jnp.concatenate(
                [acc[b * block + g * seqs : b * block + (g + 1) * seqs, :] for b in range(blocks(t))], axis=0
            )
        for k in range(1, nx):
            part_copy(t, k).start()

    def q_copy(t, d, r):
        core = lax.rem(c + r, CORES)
        if isinstance(t, int) and t >= half - 1:
            chip = z if t == half else z + half
        else:
            chip = z - 1 - t if d == 0 else z + 1 + t
        slot = 2 * (half - 1 - t) - 1 + d
        if isinstance(t, int) and t >= half - 1:
            slot = nz - 1 if t == half else 0
        return remote(
            q_send.at[t, CORES * d + core], q_in.at[slot, c], q_send_sem.at[r], q_sem.at[slot, c], at_z(chip, core)
        )

    def send_queries(t):
        rows = blocks(t) * seqs
        total = part[t, x, :rows]
        for k in range(1, nx):
            part_copy(t, k).wait_recv()
            total = total + part_in[t, k - 1, :rows]
        for b in range(blocks(t)):
            q_send[t, b] = total[b * seqs : (b + 1) * seqs, :].astype(BF16)
        for d in range(blocks(t) // CORES):
            for r in range(CORES):
                if isinstance(t, int) and t == half and r == 0:
                    q_in[nz - 1, c] = q_send[half, c]
                else:
                    q_copy(t, d, r).start()

    for j in range(IN_CHUNKS):
        for d in range(2):
            ring(d, 0, j).start()
    for j in range(IN_CHUNKS):
        ref = own_slot.at[:, piece(j)]
        remote(ref, ref, pair_send_sem.at[0, half], pair_sem.at[0, half], pair).start()
    for load in loads[2:]:
        load.start()
    wo_copy = remote(w_out.at[:, half_cols(other)], wo.at[c], wo_send_sem, wo_sem, pair)
    wo_copy.start()

    def gather_step(s):
        known = isinstance(s, int)
        before = half if known and s == 0 else s - 1
        for j in range(IN_CHUNKS):
            for d in range(2):
                if not known or travels(d, s, j):
                    ring(d, s, j).wait_recv()
                    if not known or (s < half - 1 and travels(d, s + 1, j)):
                        ring(d, s + 1, j).start()
                    to_pair(d, s, j).start()
            if known and s == 0 and j == 0:
                loads[1].wait()
            dot_piece(before, j)
        send_parts(before)
        if not known or s > 0:
            send_queries(half if known and s == 1 else s - 2)

    gather_step(0)
    gather_step(1)

    @pl.loop(2, half - 2)
    def _(s):
        gather_step(s)

    for s in range(max(half - 2, 2), half):
        gather_step(s)
    for j in range(IN_CHUNKS):
        dot_piece(half - 1, j)
    heads = CORES * feats // hd

    def scores_of(i, lo, hi):
        rows = jnp.concatenate([q_wide[lo:hi, core, i, :] for core in range(CORES)], axis=1)
        query = jnp.concatenate([rows[:, h * hd : (h + 1) * hd] for h in range(heads)], axis=0).astype(BF16)
        return lax.dot_general(query, k_buf[i], (((1,), (1,)), ((), ())), preferred_element_type=F32)

    def probs_of(i, scores):
        scores = scores * F32(hd**-0.5)
        live = lax.broadcasted_iota(jnp.int32, scores.shape, 1) < lengths[i]
        scores = jnp.where(live, scores, F32(-1e30))
        expo = jnp.where(live, jnp.exp(scores - jnp.max(scores, axis=1, keepdims=True)), F32(0.0))
        return (expo / jnp.sum(expo, axis=1, keepdims=True)).astype(BF16)

    def att_copy(v, r):
        core = lax.rem(c + r, CORES)
        slot = v if v in (0, nz - 1) else v + 1 if v % 2 else v - 1
        return remote(
            att_send.at[v, core],
            att_in.at[x, slot, c],
            att_send_sem.at[r],
            att_sem.at[slot, c],
            at_z(z + source_offset(v, half), core),
        )

    def far_copy(k, core):
        device = {**at_z(z + half, core), **at_x(k)}
        return remote(att_send.at[0, core], att_in.at[x, 0, c], far_send_sem, far_sem.at[k - 1, c], device)

    def attend(lo, hi):
        for v in range(lo, hi):
            for r in range(CORES):
                core = lax.rem(c + r, CORES)
                if v < nz - 1 or r > 0:
                    ref = q_in.at[v, core]
                    remote(ref, ref, q_send_sem.at[r], q_sem.at[v, core], pair).wait_recv()
        q_wide[lo:hi] = q_in[lo:hi].astype(F32)
        scores = [scores_of(i, lo, hi) for i in range(seqs)]
        probs = [probs_of(i, scores[i]) for i in range(seqs)]
        mixed = [jnp.dot(probs[i], v_buf[i], preferred_element_type=F32) for i in range(seqs)]
        for i in range(seqs):
            wide = jnp.concatenate(
                [mixed[i][h * (hi - lo) : (h + 1) * (hi - lo), :] for h in range(heads)], axis=1
            )
            for core in range(CORES):
                att_wide[lo:hi, core, i, :] = wide[:, core * feats : (core + 1) * feats]
        att_send[lo:hi] = att_wide[lo:hi].astype(BF16)
        for v in range(lo, hi):
            for r in range(CORES):
                if v == nz - 1 and r == 0:
                    att_in[x, v, c] = att_send[v, c]
                else:
                    att_copy(v, r).start()
                if v == 0:
                    for k in range(1, nx):
                        far_copy(k, lax.rem(c + r, CORES)).start()

    send_parts(half - 1)
    send_queries(half - 2)
    for load in loads[3:]:
        load.wait()
    send_queries(half - 1)
    attend(nz // 4, nz)
    attend(0, nz // 4)

    own_batch = nz // PER_BATCH + 1

    def batch(b):
        known = isinstance(b, int)
        if known and b in (0, own_batch):
            return (0 if b == 0 else nz - 1), 1
        return (1, 2) if known and b == 1 else (PER_BATCH * b - 5, PER_BATCH)

    def rows_copy(b, k):
        ref = att_in.at[x, pl.ds(*batch(b))]
        return remote(ref, ref, rows_send_sem.at[b, k - 1], rows_sem.at[b, k - 1], at_x(k))

    def swap_copy(b):
        ref = att.at[c, pl.ds(*batch(b))]
        return remote(ref, ref, swap_send_sem.at[b], swap_sem.at[b], pair)

    def pass_on(b):
        for k in range(1, nx):
            if isinstance(b, int) and b == 0:
                for core in range(CORES):
                    ref = att_in.at[lax.rem(x - k + nx, nx), 0, core]
                    remote(ref, ref, far_send_sem, far_sem.at[k - 1, core], pair).wait_recv()
            else:
                rows_copy(b, k).wait_recv()
        start, count = batch(b)
        for n in range(count):
            for core in range(CORES):
                v = start + n
                att[c, v, core] = jnp.concatenate(
                    [att_in[g, v, core].astype(F32) for g in range(nx)], axis=0
                ).astype(BF16)
        swap_copy(b).start()

    for b in [1, 0, *range(2, own_batch + 1)]:
        start, count = batch(b)
        for v in range(start, start + count):
            for r in range(CORES):
                core = lax.rem(c + r, CORES)
                if v < nz - 1 or r > 0:
                    ref = att_in.at[x, v, core]
                    remote(ref, ref, att_send_sem.at[r], att_sem.at[v, core], pair).wait_recv()
        if b == 0:
            pass_on(0)
        else:
            for k in range(1, nx):
                rows_copy(b, k).start()
    loads[2].wait()
    wo_copy.wait_recv()

    def out_piece(j):
        return pl.ds(j * out_cols, out_cols)

    def projected(v, count, j):
        lhs = jnp.concatenate(
            [att[f, pl.ds(v, count)].reshape(count * CORES * block, feats) for f in range(CORES)], axis=1
        )
        rhs = wo[:, :, j * out_cols : (j + 1) * out_cols].reshape(CORES * feats, out_cols)
        return jnp.dot(lhs, rhs, preferred_element_type=F32)

    def sums_copy(d, s, j):
        return remote(
            sums.at[d, s, :, out_piece(j)],
            sums_in.at[d, s, :, out_piece(j)],
            sums_send_sem.at[d, s],
            sums_sem.at[d, s, j],
            side[d],
        )

    def starts(d, j):
        return (j < (OUT_CHUNKS + 1) // 2) == (d == 0)

    tall = CORES * block

    def out_step(s):
        known = isinstance(s, int)
        for j in range(OUT_CHUNKS):
            span = slice(j * out_cols, (j + 1) * out_cols)
            if known and s == 0:
                d = 0 if starts(0, j) else 1
                sums[d, 0, :, span] = projected(0, 1, j).astype(BF16)
                sums_copy(d, 0, j).start()
                continue
            both = projected(2 * s - 1, 2, j)
            for d in range(2):
                term = both[d * tall : (d + 1) * tall]
                if not known or s > 1 or starts(d, j):
                    sums_copy(d, s - 1, j).wait_recv()
                    term = term + sums_in[d, s - 1, :, span].astype(F32)
                sums[d, s, :, span] = term.astype(BF16)
                sums_copy(d, s, j).start()

    pass_on(1)
    swap_copy(0).wait_recv()
    out_step(0)
    pass_on(2)
    swap_copy(1).wait_recv()
    out_step(1)

    @pl.loop(2, own_batch - 1)
    def _(b):
        pass_on(b + 1)
        swap_copy(b).wait_recv()
        out_step(2 * b - 2)
        out_step(2 * b - 1)

    pass_on(own_batch)
    swap_copy(own_batch - 1).wait_recv()

    @pl.loop(half - 2, half)
    def _(s):
        out_step(s)

    swap_copy(own_batch).wait_recv()

    def last_copy(j):
        own = pl.ds(pl.multiple_of(c * own_cols + j * out_cols, 128), out_cols)
        return remote(
            last.at[other, :, out_piece(j)], out.at[:, own], last_send_sem.at[j], last_sem.at[j], pair
        )

    for j in range(OUT_CHUNKS):
        span = slice(j * out_cols, (j + 1) * out_cols)
        term = projected(nz - 1, 1, j)
        for d in range(2):
            sums_copy(d, half - 1, j).wait_recv()
            term = term + sums_in[d, half - 1, :, span].astype(F32)
        for core in range(CORES):
            last[core, :, span] = term[core * block : (core + 1) * block].astype(BF16)
        last_copy(j).start()
    out[:, half_cols(c)] = last[c]
    for j in range(OUT_CHUNKS):
        last_copy(j).wait_recv()

    def left(ref, sem, recv_sem, device):
        remote(ref, ref, sem, recv_sem, device).wait_send()

    @pl.loop(0, half - 1)
    def _(t):
        for d in range(2):
            left(gathered.at[0, c], pair_send_sem.at[d, t], pair_sem.at[d, t], pair)
            left(gathered.at[0, c], ring_send_sem.at[d, t], ring_sem.at[d, t, 0], side[d])
        for k in range(1, nx):
            part_copy(t, k).wait_send()

    for t in (half - 1, half):
        left(gathered.at[0, c], pair_send_sem.at[0, t], pair_sem.at[0, t], pair)
        for k in range(1, nx):
            part_copy(t, k).wait_send()

    @pl.loop(1, half)
    def _(s):
        for d in range(2):
            left(sums.at[d, s], sums_send_sem.at[d, s], sums_sem.at[d, s, 0], side[d])

    for d in range(2):
        left(
            gathered.at[0, c, :, pl.ds(0, width // 2)], ring_send_sem.at[d, half - 1], ring_sem.at[d, half - 1, 0], side[d]
        )
        first = out_cols * sum(starts(d, j) for j in range(OUT_CHUNKS))
        left(sums.at[d, 0, :, pl.ds(0, first)], sums_send_sem.at[d, 0], sums_sem.at[d, 0, 0], side[d])
    for r in range(CORES):
        ref = q_in.at[pl.ds(0, nz - 1 + r), 0]
        left(ref, q_send_sem.at[r], q_sem.at[0, 0], pair)
        left(ref, att_send_sem.at[r], att_sem.at[0, 0], pair)
    for b in range(own_batch + 1):
        swap_copy(b).wait_send()
        if b > 0:
            for k in range(1, nx):
                rows_copy(b, k).wait_send()
    left(q_in.at[pl.ds(0, nx - 1)], far_send_sem, far_sem.at[0, 0], pair)
    wo_copy.wait_send()
    for j in range(OUT_CHUNKS):
        last_copy(j).wait_send()


def solution(mesh):
    nz = mesh.shape["gx"] // CORES
    nx = mesh.shape["gy"]
    half = nz // 2

    def body(hidden_in, w_query, w_out, cache_keys, cache_values, lengths):
        block, width = hidden_in.shape
        feats = w_query.shape[1]
        seqs, slots, hd = cache_keys.shape
        own_cols = width // CORES
        dma = pltpu.SemaphoreType.DMA
        hbm = pl.BlockSpec(memory_space=pltpu.HBM)
        return pl.pallas_call(
            functools.partial(kernel, nz, nx),
            out_shape=jax.ShapeDtypeStruct((block, width), BF16),
            in_specs=[pl.BlockSpec(memory_space=pltpu.SMEM)] + [hbm] * 5,
            out_specs=pl.BlockSpec(memory_space=pltpu.VMEM),
            scratch_shapes=[
                pltpu.VMEM((half + 1, 2 * CORES, block, width), BF16),
                pltpu.VMEM(w_query.shape, BF16),
                pltpu.VMEM((CORES, feats, own_cols), BF16),
                pltpu.VMEM(cache_keys.shape, BF16),
                pltpu.VMEM(cache_values.shape, BF16),
                pltpu.VMEM((2 * CORES * block, feats), F32),
                pltpu.VMEM((half + 1, nx, 2 * CORES * seqs, feats), F32),
                pltpu.VMEM((half + 1, nx - 1, 2 * CORES * seqs, feats), F32),
                pltpu.VMEM((half + 1, 2 * CORES, seqs, feats), BF16),
                pltpu.VMEM((nz, CORES, seqs, feats), BF16),
                pltpu.VMEM((nz, CORES, seqs, feats), F32),
                pltpu.VMEM((nz, CORES, seqs, feats), F32),
                pltpu.VMEM((nz, CORES, seqs, feats), BF16),
                pltpu.VMEM((nx, nz, CORES, seqs, feats), BF16),
                pltpu.VMEM((CORES, nz, CORES, block, feats), BF16),
                pltpu.VMEM((2, half, CORES * block, own_cols), BF16),
                pltpu.VMEM((2, half, CORES * block, own_cols), BF16),
                pltpu.VMEM((CORES, block, own_cols), BF16),
                dma((5,)),
                dma((2, half)),
                dma((2, half, IN_CHUNKS)),
                dma((2, half + 1)),
                dma((2, half + 1)),
                dma((half + 1, nx - 1)),
                dma((half + 1, nx - 1)),
                dma((CORES,)),
                dma((nz, CORES)),
                dma((CORES,)),
                dma((nz, CORES)),
                dma(()),
                dma((nx - 1, CORES)),
                dma((nz // PER_BATCH + 2, nx - 1)),
                dma((nz // PER_BATCH + 2, nx - 1)),
                dma((nz // PER_BATCH + 2,)),
                dma((nz // PER_BATCH + 2,)),
                dma(()),
                dma(()),
                dma((2, half)),
                dma((2, half, OUT_CHUNKS)),
                dma((OUT_CHUNKS,)),
                dma((OUT_CHUNKS,)),
            ],
            compiler_params=pltpu.CompilerParams(
                collective_id=0, has_side_effects=True, vmem_limit_bytes=215 * 2**18
            ),
            name="decode_step",
        )(lengths, hidden_in, w_query, w_out, cache_keys, cache_values)

    return jax.shard_map(
        body,
        mesh=mesh,
        in_specs=(
            P(("groups", "gx"), "gy"),
            P("gy", "gx"),
            P("gx", "gy"),
            P(("groups", "gx", "gy"), None, None),
            P(("groups", "gx", "gy"), None, None),
            P(("groups", "gx", "gy")),
        ),
        out_specs=P(("groups", "gx"), "gy"),
        check_vma=False,
    )
```

```python
import functools

import jax
import jax.numpy as jnp
from jax import lax
from jax.experimental import pallas as pl
from jax.experimental.pallas import tpu as pltpu
from jax.sharding import PartitionSpec as P

MESH = pl.DeviceIdType.MESH
CORES = 2
IN_CHUNKS = 6
OUT_CHUNKS = 6
PER_BATCH = 4
F32 = jnp.float32
BF16 = jnp.bfloat16


def source_offset(v, half):
    return half - (v + 1) // 2 if v % 2 else half + v // 2


def kernel(
    nz,
    nx,
    lengths,
    hidden,
    w_query,
    w_out,
    keys,
    values,
    out,
    gathered,
    wq,
    wo,
    k_buf,
    v_buf,
    acc,
    part,
    part_in,
    q_send,
    q_in,
    q_wide,
    att_wide,
    att_send,
    att_in,
    att,
    sums,
    sums_in,
    last,
    local_sem,
    ring_send_sem,
    ring_sem,
    pair_send_sem,
    pair_sem,
    part_send_sem,
    part_sem,
    q_send_sem,
    q_sem,
    att_send_sem,
    att_sem,
    far_send_sem,
    far_sem,
    rows_send_sem,
    rows_sem,
    swap_send_sem,
    swap_sem,
    wo_send_sem,
    wo_sem,
    sums_send_sem,
    sums_sem,
    last_send_sem,
    last_sem,
):
    half = nz // 2
    gx = lax.axis_index("gx")
    x = lax.axis_index("gy")
    z = gx // CORES
    c = gx % CORES
    other = 1 - c
    seqs, slots, hd = k_buf.shape
    width = hidden.shape[1]
    cols = width // IN_CHUNKS
    own_cols = width // CORES
    out_cols = own_cols // OUT_CHUNKS
    feats = w_query.shape[1]
    block = nx * seqs

    def at_z(chip, core):
        return {"gx": lax.rem(chip + 2 * nz, nz) * CORES + core}

    def at_x(offset):
        return {"gy": lax.rem(x + offset, nx)}

    side = (at_z(z + 1, c), at_z(z - 1, c))
    pair = {"gx": z * CORES + other}

    def remote(src, dst, send_sem, recv_sem, device):
        return pltpu.make_async_remote_copy(
            src_ref=src, dst_ref=dst, send_sem=send_sem, recv_sem=recv_sem, device_id=device, device_id_type=MESH
        )

    def half_cols(core):
        return pl.ds(pl.multiple_of(core * own_cols, 128), own_cols)

    own_slot = gathered.at[half, c]
    loads = [
        pltpu.make_async_copy(hidden, own_slot, local_sem.at[0]),
        pltpu.make_async_copy(w_query, wq, local_sem.at[1]),
        pltpu.make_async_copy(w_out.at[:, half_cols(c)], wo.at[c], local_sem.at[2]),
        pltpu.make_async_copy(keys, k_buf, local_sem.at[3]),
        pltpu.make_async_copy(values, v_buf, local_sem.at[4]),
    ]
    loads[0].start()
    loads[1].start()

    barrier = pltpu.get_barrier_semaphore()
    greeted = [*side, pair] + [at_x(k) for k in range(1, nx)]
    for device in greeted:
        pl.semaphore_signal(barrier, inc=1, device_id=device, device_id_type=MESH)
    pl.semaphore_wait(barrier, len(greeted))
    loads[0].wait()

    def piece(j):
        return pl.ds(j * cols, cols)

    def home(s, d):
        return 0 if isinstance(s, int) and s == half - 1 else d

    def ring(d, s, j):
        src = own_slot if isinstance(s, int) and s == 0 else gathered.at[s - 1, CORES * d + c]
        dst = gathered.at[s, CORES * home(s, d) + c]
        return remote(src.at[:, piece(j)], dst.at[:, piece(j)], ring_send_sem.at[d, s], ring_sem.at[d, s, j], side[d])

    def to_pair(d, s, j):
        ref = gathered.at[s, CORES * home(s, d) + c, :, piece(j)]
        return remote(ref, ref, pair_send_sem.at[home(s, d), s], pair_sem.at[home(s, d), s], pair)

    def travels(d, s, j):
        return s < half - 1 or (j < IN_CHUNKS // 2) == (d == 0)

    def blocks(t):
        return CORES if isinstance(t, int) and t >= half - 1 else 2 * CORES

    def dot_piece(t, j):
        if j == 0:
            for d in range(blocks(t) // CORES):
                ref = gathered.at[t, CORES * d + other]
                remote(ref, ref, pair_send_sem.at[d, t], pair_sem.at[d, t], pair).wait_recv()
        tall = blocks(t) * block
        lhs = gathered[t, : blocks(t), :, j * cols : (j + 1) * cols].reshape(tall, cols)
        term = jnp.dot(lhs, wq[j * cols : (j + 1) * cols, :], preferred_element_type=F32)
        if j == 0:
            acc[:tall] = term
        else:
            acc[:tall] += term

    def part_copy(t, k):
        rows = pl.ds(0, blocks(t) * seqs)
        return remote(
            part.at[t, lax.rem(x + k, nx), rows],
            part_in.at[t, k - 1, rows],
            part_send_sem.at[t, k - 1],
            part_sem.at[t, k - 1],
            at_x(k),
        )

    def send_parts(t):
        for g in range(nx):
            part[t, g, : blocks(t) * seqs] = jnp.concatenate(
                [acc[b * block + g * seqs : b * block + (g + 1) * seqs, :] for b in range(blocks(t))], axis=0
            )
        for k in range(1, nx):
            part_copy(t, k).start()

    def q_copy(t, d, r):
        core = lax.rem(c + r, CORES)
        if isinstance(t, int) and t >= half - 1:
            chip = z if t == half else z + half
        else:
            chip = z - 1 - t if d == 0 else z + 1 + t
        slot = 2 * (half - 1 - t) - 1 + d
        if isinstance(t, int) and t >= half - 1:
            slot = nz - 1 if t == half else 0
        return remote(
            q_send.at[t, CORES * d + core], q_in.at[slot, c], q_send_sem.at[r], q_sem.at[slot, c], at_z(chip, core)
        )

    def send_queries(t):
        rows = blocks(t) * seqs
        total = part[t, x, :rows]
        for k in range(1, nx):
            part_copy(t, k).wait_recv()
            total = total + part_in[t, k - 1, :rows]
        for b in range(blocks(t)):
            q_send[t, b] = total[b * seqs : (b + 1) * seqs, :].astype(BF16)
        for d in range(blocks(t) // CORES):
            for r in range(CORES):
                if isinstance(t, int) and t == half and r == 0:
                    q_in[nz - 1, c] = q_send[half, c]
                else:
                    q_copy(t, d, r).start()

    for j in range(IN_CHUNKS):
        for d in range(2):
            ring(d, 0, j).start()
    for j in range(IN_CHUNKS):
        ref = own_slot.at[:, piece(j)]
        remote(ref, ref, pair_send_sem.at[0, half], pair_sem.at[0, half], pair).start()
    for load in loads[2:]:
        load.start()
    wo_copy = remote(w_out.at[:, half_cols(other)], wo.at[c], wo_send_sem, wo_sem, pair)
    wo_copy.start()

    def gather_step(s):
        known = isinstance(s, int)
        before = half if known and s == 0 else s - 1
        for j in range(IN_CHUNKS):
            for d in range(2):
                if not known or travels(d, s, j):
                    ring(d, s, j).wait_recv()
                    if not known or (s < half - 1 and travels(d, s + 1, j)):
                        ring(d, s + 1, j).start()
                    to_pair(d, s, j).start()
            if known and s == 0 and j == 0:
                loads[1].wait()
            dot_piece(before, j)
        send_parts(before)
        if not known or s > 0:
            send_queries(half if known and s == 1 else s - 2)

    gather_step(0)
    gather_step(1)

    @pl.loop(2, half - 2)
    def _(s):
        gather_step(s)

    for s in range(max(half - 2, 2), half):
        gather_step(s)
    for j in range(IN_CHUNKS):
        dot_piece(half - 1, j)
    heads = CORES * feats // hd

    def scores_of(i, lo, hi):
        rows = jnp.concatenate([q_wide[lo:hi, core, i, :] for core in range(CORES)], axis=1)
        query = jnp.concatenate([rows[:, h * hd : (h + 1) * hd] for h in range(heads)], axis=0).astype(BF16)
        return lax.dot_general(query, k_buf[i], (((1,), (1,)), ((), ())), preferred_element_type=F32)

    def probs_of(i, scores):
        scores = scores * F32(hd**-0.5)
        live = lax.broadcasted_iota(jnp.int32, scores.shape, 1) < lengths[i]
        scores = jnp.where(live, scores, F32(-1e30))
        expo = jnp.where(live, jnp.exp(scores - jnp.max(scores, axis=1, keepdims=True)), F32(0.0))
        return (expo / jnp.sum(expo, axis=1, keepdims=True)).astype(BF16)

    def att_copy(v, r):
        core = lax.rem(c + r, CORES)
        slot = v if v in (0, nz - 1) else v + 1 if v % 2 else v - 1
        return remote(
            att_send.at[v, core],
            att_in.at[x, slot, c],
            att_send_sem.at[r],
            att_sem.at[slot, c],
            at_z(z + source_offset(v, half), core),
        )

    def far_copy(k, core):
        device = {**at_z(z + half, core), **at_x(k)}
        return remote(att_send.at[0, core], att_in.at[x, 0, c], far_send_sem, far_sem.at[k - 1, c], device)

    def attend(lo, hi):
        for v in range(lo, hi):
            for r in range(CORES):
                core = lax.rem(c + r, CORES)
                if v < nz - 1 or r > 0:
                    ref = q_in.at[v, core]
                    remote(ref, ref, q_send_sem.at[r], q_sem.at[v, core], pair).wait_recv()
        q_wide[lo:hi] = q_in[lo:hi].astype(F32)
        scores = [scores_of(i, lo, hi) for i in range(seqs)]
        probs = [probs_of(i, scores[i]) for i in range(seqs)]
        mixed = [jnp.dot(probs[i], v_buf[i], preferred_element_type=F32) for i in range(seqs)]
        for i in range(seqs):
            wide = jnp.concatenate(
                [mixed[i][h * (hi - lo) : (h + 1) * (hi - lo), :] for h in range(heads)], axis=1
            )
            for core in range(CORES):
                att_wide[lo:hi, core, i, :] = wide[:, core * feats : (core + 1) * feats]
        att_send[lo:hi] = att_wide[lo:hi].astype(BF16)
        for v in range(lo, hi):
            for r in range(CORES):
                if v == nz - 1 and r == 0:
                    att_in[x, v, c] = att_send[v, c]
                else:
                    att_copy(v, r).start()
                if v == 0:
                    for k in range(1, nx):
                        far_copy(k, lax.rem(c + r, CORES)).start()

    send_parts(half - 1)
    send_queries(half - 2)
    for load in loads[3:]:
        load.wait()
    send_queries(half - 1)
    attend(nz // 4, nz)
    attend(0, nz // 4)

    own_batch = nz // PER_BATCH + 1

    def batch(b):
        known = isinstance(b, int)
        if known and b in (0, own_batch):
            return (0 if b == 0 else nz - 1), 1
        return (1, 2) if known and b == 1 else (PER_BATCH * b - 5, PER_BATCH)

    def rows_copy(b, k):
        ref = att_in.at[x, pl.ds(*batch(b))]
        return remote(ref, ref, rows_send_sem.at[b, k - 1], rows_sem.at[b, k - 1], at_x(k))

    def swap_copy(b):
        ref = att.at[c, pl.ds(*batch(b))]
        return remote(ref, ref, swap_send_sem.at[b], swap_sem.at[b], pair)

    def pass_on(b):
        for k in range(1, nx):
            if isinstance(b, int) and b == 0:
                for core in range(CORES):
                    ref = att_in.at[lax.rem(x - k + nx, nx), 0, core]
                    remote(ref, ref, far_send_sem, far_sem.at[k - 1, core], pair).wait_recv()
            else:
                rows_copy(b, k).wait_recv()
        start, count = batch(b)
        for n in range(count):
            for core in range(CORES):
                v = start + n
                att[c, v, core] = jnp.concatenate(
                    [att_in[g, v, core].astype(F32) for g in range(nx)], axis=0
                ).astype(BF16)
        swap_copy(b).start()

    for b in [*range(3, own_batch + 1), 1, 2, 0]:
        start, count = batch(b)
        for v in range(start, start + count):
            for r in range(CORES):
                core = lax.rem(c + r, CORES)
                if v < nz - 1 or r > 0:
                    ref = att_in.at[x, v, core]
                    remote(ref, ref, att_send_sem.at[r], att_sem.at[v, core], pair).wait_recv()
        if b == 0:
            pass_on(0)
        else:
            for k in range(1, nx):
                rows_copy(b, k).start()
    loads[2].wait()
    wo_copy.wait_recv()

    def out_piece(j):
        return pl.ds(j * out_cols, out_cols)

    def projected(v, count, j):
        lhs = jnp.concatenate(
            [att[f, pl.ds(v, count)].reshape(count * CORES * block, feats) for f in range(CORES)], axis=1
        )
        rhs = wo[:, :, j * out_cols : (j + 1) * out_cols].reshape(CORES * feats, out_cols)
        return jnp.dot(lhs, rhs, preferred_element_type=F32)

    def sums_copy(d, s, j):
        return remote(
            sums.at[d, s, :, out_piece(j)],
            sums_in.at[d, s, :, out_piece(j)],
            sums_send_sem.at[d, s],
            sums_sem.at[d, s, j],
            side[d],
        )

    def starts(d, j):
        return (j < (OUT_CHUNKS + 1) // 2) == (d == 0)

    tall = CORES * block

    def out_step(s):
        known = isinstance(s, int)
        for j in range(OUT_CHUNKS):
            span = slice(j * out_cols, (j + 1) * out_cols)
            if known and s == 0:
                d = 0 if starts(0, j) else 1
                sums[d, 0, :, span] = projected(0, 1, j).astype(BF16)
                sums_copy(d, 0, j).start()
                continue
            both = projected(2 * s - 1, 2, j)
            for d in range(2):
                term = both[d * tall : (d + 1) * tall]
                if not known or s > 1 or starts(d, j):
                    sums_copy(d, s - 1, j).wait_recv()
                    term = term + sums_in[d, s - 1, :, span].astype(F32)
                sums[d, s, :, span] = term.astype(BF16)
                sums_copy(d, s, j).start()

    pass_on(1)
    swap_copy(0).wait_recv()
    out_step(0)
    pass_on(2)
    swap_copy(1).wait_recv()
    out_step(1)

    @pl.loop(2, own_batch - 1)
    def _(b):
        pass_on(b + 1)
        swap_copy(b).wait_recv()
        out_step(2 * b - 2)
        out_step(2 * b - 1)

    pass_on(own_batch)
    swap_copy(own_batch - 1).wait_recv()

    @pl.loop(half - 2, half)
    def _(s):
        out_step(s)

    swap_copy(own_batch).wait_recv()

    def last_copy(j):
        own = pl.ds(pl.multiple_of(c * own_cols + j * out_cols, 128), out_cols)
        return remote(
            last.at[other, :, out_piece(j)], out.at[:, own], last_send_sem.at[j], last_sem.at[j], pair
        )

    for j in range(OUT_CHUNKS):
        span = slice(j * out_cols, (j + 1) * out_cols)
        term = projected(nz - 1, 1, j)
        for d in range(2):
            sums_copy(d, half - 1, j).wait_recv()
            term = term + sums_in[d, half - 1, :, span].astype(F32)
        for core in range(CORES):
            last[core, :, span] = term[core * block : (core + 1) * block].astype(BF16)
        last_copy(j).start()
    out[:, half_cols(c)] = last[c]
    for j in range(OUT_CHUNKS):
        last_copy(j).wait_recv()

    def left(ref, sem, recv_sem, device):
        remote(ref, ref, sem, recv_sem, device).wait_send()

    @pl.loop(0, half - 1)
    def _(t):
        for d in range(2):
            left(gathered.at[0, c], pair_send_sem.at[d, t], pair_sem.at[d, t], pair)
            left(gathered.at[0, c], ring_send_sem.at[d, t], ring_sem.at[d, t, 0], side[d])
        for k in range(1, nx):
            part_copy(t, k).wait_send()

    for t in (half - 1, half):
        left(gathered.at[0, c], pair_send_sem.at[0, t], pair_sem.at[0, t], pair)
        for k in range(1, nx):
            part_copy(t, k).wait_send()

    @pl.loop(1, half)
    def _(s):
        for d in range(2):
            left(sums.at[d, s], sums_send_sem.at[d, s], sums_sem.at[d, s, 0], side[d])

    for d in range(2):
        left(
            gathered.at[0, c, :, pl.ds(0, width // 2)], ring_send_sem.at[d, half - 1], ring_sem.at[d, half - 1, 0], side[d]
        )
        first = out_cols * sum(starts(d, j) for j in range(OUT_CHUNKS))
        left(sums.at[d, 0, :, pl.ds(0, first)], sums_send_sem.at[d, 0], sums_sem.at[d, 0, 0], side[d])
    for r in range(CORES):
        ref = q_in.at[pl.ds(0, nz - 1 + r), 0]
        left(ref, q_send_sem.at[r], q_sem.at[0, 0], pair)
        left(ref, att_send_sem.at[r], att_sem.at[0, 0], pair)
    for b in range(own_batch + 1):
        swap_copy(b).wait_send()
        if b > 0:
            for k in range(1, nx):
                rows_copy(b, k).wait_send()
    left(q_in.at[pl.ds(0, nx - 1)], far_send_sem, far_sem.at[0, 0], pair)
    wo_copy.wait_send()
    for j in range(OUT_CHUNKS):
        last_copy(j).wait_send()


def solution(mesh):
    nz = mesh.shape["gx"] // CORES
    nx = mesh.shape["gy"]
    half = nz // 2

    def body(hidden_in, w_query, w_out, cache_keys, cache_values, lengths):
        block, width = hidden_in.shape
        feats = w_query.shape[1]
        seqs, slots, hd = cache_keys.shape
        own_cols = width // CORES
        dma = pltpu.SemaphoreType.DMA
        hbm = pl.BlockSpec(memory_space=pltpu.HBM)
        return pl.pallas_call(
            functools.partial(kernel, nz, nx),
            out_shape=jax.ShapeDtypeStruct((block, width), BF16),
            in_specs=[pl.BlockSpec(memory_space=pltpu.SMEM)] + [hbm] * 5,
            out_specs=pl.BlockSpec(memory_space=pltpu.VMEM),
            scratch_shapes=[
                pltpu.VMEM((half + 1, 2 * CORES, block, width), BF16),
                pltpu.VMEM(w_query.shape, BF16),
                pltpu.VMEM((CORES, feats, own_cols), BF16),
                pltpu.VMEM(cache_keys.shape, BF16),
                pltpu.VMEM(cache_values.shape, BF16),
                pltpu.VMEM((2 * CORES * block, feats), F32),
                pltpu.VMEM((half + 1, nx, 2 * CORES * seqs, feats), F32),
                pltpu.VMEM((half + 1, nx - 1, 2 * CORES * seqs, feats), F32),
                pltpu.VMEM((half + 1, 2 * CORES, seqs, feats), BF16),
                pltpu.VMEM((nz, CORES, seqs, feats), BF16),
                pltpu.VMEM((nz, CORES, seqs, feats), F32),
                pltpu.VMEM((nz, CORES, seqs, feats), F32),
                pltpu.VMEM((nz, CORES, seqs, feats), BF16),
                pltpu.VMEM((nx, nz, CORES, seqs, feats), BF16),
                pltpu.VMEM((CORES, nz, CORES, block, feats), BF16),
                pltpu.VMEM((2, half, CORES * block, own_cols), BF16),
                pltpu.VMEM((2, half, CORES * block, own_cols), BF16),
                pltpu.VMEM((CORES, block, own_cols), BF16),
                dma((5,)),
                dma((2, half)),
                dma((2, half, IN_CHUNKS)),
                dma((2, half + 1)),
                dma((2, half + 1)),
                dma((half + 1, nx - 1)),
                dma((half + 1, nx - 1)),
                dma((CORES,)),
                dma((nz, CORES)),
                dma((CORES,)),
                dma((nz, CORES)),
                dma(()),
                dma((nx - 1, CORES)),
                dma((nz // PER_BATCH + 2, nx - 1)),
                dma((nz // PER_BATCH + 2, nx - 1)),
                dma((nz // PER_BATCH + 2,)),
                dma((nz // PER_BATCH + 2,)),
                dma(()),
                dma(()),
                dma((2, half)),
                dma((2, half, OUT_CHUNKS)),
                dma((OUT_CHUNKS,)),
                dma((OUT_CHUNKS,)),
            ],
            compiler_params=pltpu.CompilerParams(
                collective_id=0, has_side_effects=True, vmem_limit_bytes=215 * 2**18
            ),
            name="decode_step",
        )(lengths, hidden_in, w_query, w_out, cache_keys, cache_values)

    return jax.shard_map(
        body,
        mesh=mesh,
        in_specs=(
            P(("groups", "gx"), "gy"),
            P("gy", "gx"),
            P("gx", "gy"),
            P(("groups", "gx", "gy"), None, None),
            P(("groups", "gx", "gy"), None, None),
            P(("groups", "gx", "gy")),
        ),
        out_specs=P(("groups", "gx"), "gy"),
        check_vma=False,
    )
```
